32 devices in a mesh: dp: 8 (over z, core), tensor: 4 (over y, x).
Axes of the slice: x: 2, y: 2, z: 4, core: 2. Of those that a mesh axis runs over, the one named last changes fastest.
Arguments:
- activations: bfloat16 [18432, 8192], P('dp', 'tensor'), may hold values from -6 to 6
- out_grads: bfloat16 [18432, 28672], P('dp', 'tensor'), may hold values from -0.078125 to 0.078125
- basis: bfloat16 [8192, 256], P('tensor'), may hold values from -0.375 to 0.375
- first_moment: float32 [256, 28672], P('dp', 'tensor'), may hold values from -6 to 6
- second_moment: float32 [256, 28672], P('dp', 'tensor'), may hold values from 0.05 to 0.8
- reward_codes: int32 [18432], P('dp'), may hold values from 0 to 15
- token_ids: int32 [18432], P('dp'), may hold values from 0 to 128004, as said below
Outputs:
- new_first: float32 [256, 28672], P('dp', 'tensor')
- new_second: float32 [256, 28672], P('dp', 'tensor')
- weight_update: bfloat16 [8192, 28672], P('dp', 'tensor')
The draws below stay inside these ranges and needn't reach their ends.
Inputs may be any that keep to these rules, and one draw needn't show every extreme that they name: `token_ids`: the id 128004 is the padding token; the first of each 2304 consecutive tokens is never padding.
All inputs are finite; a program needn't handle non-finite values.
Results may differ from the reference program's by a relative error of at most 0.019.
Values may be sent and summed in bfloat16 or wider, within the bound.
No kernel may reach another device: no remote copies, remote signals or barrier semaphores. Data moves between devices by JAX's collectives and lax.ppermute only.
A program may use at most 128 MiB of HBM per device.

```python
import math
import jax
import jax.numpy as jnp
from jax import lax

D = 8192
FF = 28672
R = 256
TOK_DEV = 2304
LEVELS = 16
ADAM_STEP = 100
TOKENS = 18432
N_TENSOR = 4


pad_token = 128004


def draw_reward_codes(key, part):
    code_key = jax.random.fold_in(key, 7)
    positions = jnp.arange(TOKENS, dtype=jnp.int32)
    block_count = TOKENS // TOK_DEV
    block_index = positions // TOK_DEV
    baseline = jax.random.randint(code_key, (TOKENS,), 0, LEVELS // 2, dtype=jnp.int32)
    ramp = block_index * (LEVELS // 2) // max(block_count - 1, 1)
    return (baseline + ramp).astype(jnp.int32)


def draw_token_ids(key, part):
    id_key = jax.random.fold_in(key, 11)
    mask_key = jax.random.fold_in(key, 12)
    rate_key = jax.random.fold_in(key, 13)
    positions = jnp.arange(TOKENS, dtype=jnp.int32)
    block_count = TOKENS // TOK_DEV
    block_index = positions // TOK_DEV
    block_rates = jax.random.randint(rate_key, (block_count,), 0, 9, dtype=jnp.int32)
    token_rates = jnp.take(block_rates, block_index)
    plain_ids = jax.random.randint(id_key, (TOKENS,), 0, pad_token, dtype=jnp.int32)
    chosen = jax.random.randint(mask_key, (TOKENS,), 0, 16, dtype=jnp.int32) < token_rates
    padded = chosen & (positions % TOK_DEV != 0)
    return jnp.where(padded, pad_token, plain_ids).astype(jnp.int32)


def block_scale(stream_key, extent, shards, smallest, largest):
    def one(dim, blocks):
        heights = jax.random.uniform(jax.random.fold_in(jax.random.fold_in(stream_key, 6), dim), (blocks,), jnp.float32, smallest / len(shards), largest / len(shards))
        return jnp.repeat(jnp.exp(heights), extent[dim] // blocks).reshape((-1,) + (1,) * (len(extent) - dim - 1))

    factor_of = one(*shards[0])
    for cut in shards[1:]:
        factor_of = factor_of * one(*cut)
    return factor_of


def noise(rng, dims, deviation, bound, shards=(), kind=jnp.bfloat16):
    array = deviation * jax.random.normal(rng, dims, jnp.float32)
    if shards:
        array = array * block_scale(rng, dims, shards, -0.22, 0.18)
    return jnp.clip(array, -bound, bound).astype(kind)


def setup_inputs(seed: int = 0) -> dict:
    seeds = jax.random.split(jax.random.key(seed), 8)
    return {
        "activations": noise(seeds[0], (TOKENS, D), 1.0, 6.0, ((0, 8), (1, 4))),
        "out_grads": noise(seeds[1], (TOKENS, FF), (4 * (D * TOKENS // R) ** -0.5), 0.078125, ((0, 8), (1, 4))),
        "basis": noise(seeds[2], (D, R), R ** -0.5, 0.375, ((0, 4),)),
        "first_moment": noise(seeds[3], (R, FF), 1.0, 6.0, ((0, 8), (1, 4)), jnp.float32),
        "second_moment": jnp.clip(jnp.exp(math.log(0.8) - 2.7725887 * jax.random.uniform(seeds[4], (R, FF), jnp.float32) ** block_scale(seeds[4], (R, FF), ((0, 8), (1, 4)), -0.2, 0.2)), 0.05, 0.8),
        "reward_codes": draw_reward_codes(jax.random.fold_in(seeds[7], 71), 0),
        "token_ids": draw_token_ids(jax.random.fold_in(seeds[7], 71), 0),
    }


pad_token = 128004
reward_temp = 0.2
beta_one = 0.9
beta_two = 0.999
adam_eps = 1e-08

def reference(activations, out_grads, basis, first_moment, second_moment, reward_codes, token_ids):
    block_width = D // N_TENSOR
    projected = jnp.zeros((TOKENS, R), jnp.float32)
    for position in range(N_TENSOR):
        lower = position * block_width
        part_sum = jnp.dot(activations[:, lower:lower + block_width], basis[lower:lower + block_width, :], preferred_element_type=jnp.float32)
        rounded = lax.optimization_barrier(part_sum.astype(jnp.bfloat16))
        projected = projected + rounded.astype(jnp.float32)
    unmasked = (token_ids != pad_token).astype(jnp.float32)
    weights = unmasked * jnp.exp(reward_temp * reward_codes.astype(jnp.float32))
    normalizer = jnp.sum(weights)
    weighted = (weights[:, None] * projected).astype(jnp.bfloat16)
    raw_gradient = lax.dot_general(weighted, out_grads, (((0,), (0,)), ((), ())), preferred_element_type=jnp.float32)
    gradient = raw_gradient * (TOKENS / normalizer)
    new_first = beta_one * first_moment + (1.0 - beta_one) * gradient
    new_second = beta_two * second_moment + (1.0 - beta_two) * gradient * gradient
    bias_one = 1.0 - beta_one ** ADAM_STEP
    bias_two = 1.0 - beta_two ** ADAM_STEP
    update = (new_first / bias_one / (jnp.sqrt(new_second / bias_two) + adam_eps)).astype(jnp.bfloat16)
    weight_update = jnp.dot(basis, update, preferred_element_type=jnp.float32).astype(jnp.bfloat16)
    return (new_first, new_second, weight_update)
```

```python
import functools

import jax
import jax.numpy as jnp
from jax import lax
from jax.experimental import pallas as pl
from jax.experimental.pallas import tpu as pltpu
from jax.sharding import PartitionSpec as P

ADAM_STEP = 100


pad_token = 128004
reward_temp = 0.2
beta_one = 0.9
beta_two = 0.999
adam_eps = 1e-08

bias_one = 1.0 - beta_one**ADAM_STEP
bias_two = 1.0 - beta_two**ADAM_STEP

F32, BF16 = jnp.float32, jnp.bfloat16
CORES = 2
CHUNKS = (4, 4, 3, 3)
MIB = 1 << 20


def from_root(block, axis, owner):
    block = jnp.where(lax.axis_index(axis) == owner, block, jnp.zeros_like(block))
    return lax.psum(block, axis)


def local_general(activations, out_grads, basis, first_moment, second_moment, reward_codes, token_ids):
    data_count = lax.axis_size("dp")
    tensor_count = lax.axis_size("tensor")
    partial_value = jnp.dot(activations, basis, preferred_element_type=jnp.float32)
    projected = lax.psum(partial_value.astype(jnp.bfloat16), "tensor").astype(jnp.float32)
    unmasked = (token_ids != pad_token).astype(jnp.float32)
    weights = unmasked * jnp.exp(reward_temp * reward_codes.astype(jnp.float32))
    local_total = jnp.sum(weights)
    weighted = (weights[:, None] * projected).astype(jnp.bfloat16)
    raw_grad = lax.dot_general(
        weighted, out_grads, (((0,), (0,)), ((), ())), preferred_element_type=jnp.float32
    )
    normalizer = lax.psum(local_total, "dp")
    grad_rows = lax.psum_scatter(
        raw_grad.astype(jnp.bfloat16), "dp", scatter_dimension=0, tiled=True
    ).astype(jnp.float32)
    token_count = activations.shape[0] * data_count
    gradient = grad_rows * (token_count / normalizer)
    new_first = beta_one * first_moment + (1.0 - beta_one) * gradient
    new_second = beta_two * second_moment + (1.0 - beta_two) * gradient * gradient
    update = (new_first / bias_one / (jnp.sqrt(new_second / bias_two) + adam_eps)).astype(
        jnp.bfloat16
    )
    row_count = basis.shape[0] * tensor_count // data_count
    data_index = lax.axis_index("dp")
    owner_index = data_index * tensor_count // data_count
    owner_rows = from_root(basis, "tensor", owner_index)
    offset = data_index % (data_count // tensor_count) * row_count
    basis_rows = lax.dynamic_slice_in_dim(owner_rows, offset, row_count, 0)
    summed = jnp.dot(
        basis_rows,
        lax.all_gather(update, "dp", axis=0, tiled=True),
        preferred_element_type=jnp.float32,
    )
    return (new_first, new_second, summed.astype(jnp.bfloat16))


def pick(value, width):
    best = 128
    for w in range(128, width + 1, 128):
        if value % w == 0:
            best = w
    return best


def params(limit_mib):
    return pltpu.CompilerParams(
        dimension_semantics=("arbitrary",), vmem_limit_bytes=limit_mib * MIB
    )


def project_kernel(slot_ref, basis_ref, act_ref, out_ref, turned):
    rows = basis_ref.shape[1] // slot_ref.shape[0]

    @pl.when(pl.program_id(0) == 0)
    def _():
        flipped = basis_ref[...].T
        for n in range(slot_ref.shape[0]):
            at = pl.multiple_of(slot_ref[n] * rows, rows)
            turned[pl.ds(at, rows), :] = flipped[n * rows : (n + 1) * rows, :]

    out_ref[...] = lax.dot_general(
        turned[...], act_ref[...], (((1,), (1,)), ((), ())), preferred_element_type=F32
    ).astype(out_ref.dtype)


def project(slots, basis, activations, start, count):
    depth, rank = basis.shape
    block = pick(count, 384)
    return pl.pallas_call(
        project_kernel,
        out_shape=jax.ShapeDtypeStruct((rank, count), BF16),
        grid_spec=pltpu.PrefetchScalarGridSpec(
            num_scalar_prefetch=1,
            grid=(count // block,),
            in_specs=[
                pl.BlockSpec((depth, rank), lambda i, s: (0, 0)),
                pl.BlockSpec((block, depth), lambda i, s: (start // block + i, 0)),
            ],
            out_specs=pl.BlockSpec((rank, block), lambda i, s: (0, i)),
            scratch_shapes=[pltpu.VMEM((rank, depth), BF16)],
        ),
        compiler_params=params(20),
        cost_estimate=pl.CostEstimate(
            flops=2 * depth * rank * count,
            bytes_accessed=2 * (depth * rank + depth * count + rank * count),
            transcendentals=0,
        ),
        name="project",
    )(slots, basis, activations)


def gradient_kernel(left_a, left_b, grads_ref, keep_ref, give_ref):
    half = left_a.shape[1]
    total = jnp.dot(left_a[...], grads_ref[:half, :], preferred_element_type=F32)
    total += jnp.dot(left_b[...], grads_ref[half:, :], preferred_element_type=F32)
    rows = keep_ref.shape[0]
    keep_ref[...] = total[:rows].astype(BF16)
    give_ref[...] = total[rows:].astype(BF16)


def gradient_chunk(left_a, left_b, out_grads, start, width):
    rank, half = left_a.shape
    tokens = out_grads.shape[0]
    tile = pick(width, 512)
    while start % tile:
        tile -= 128
    return pl.pallas_call(
        gradient_kernel,
        out_shape=[jax.ShapeDtypeStruct((rank // 2, width), BF16)] * 2,
        grid=(width // tile,),
        in_specs=[
            pl.BlockSpec((rank, half), lambda i: (0, 0)),
            pl.BlockSpec((rank, half), lambda i: (0, 0)),
            pl.BlockSpec((tokens, tile), lambda i: (0, start // tile + i)),
        ],
        out_specs=[pl.BlockSpec((rank // 2, tile), lambda i: (0, i))] * 2,
        compiler_params=params(20),
        cost_estimate=pl.CostEstimate(
            flops=2 * rank * tokens * width,
            bytes_accessed=2 * (rank * tokens + tokens * width + rank * width),
            transcendentals=0,
        ),
        name="gradient",
    )(left_a, left_b, out_grads)


def moments(gradient, first, second):
    new_first = beta_one * first + (1.0 - beta_one) * gradient
    new_second = beta_two * second + (1.0 - beta_two) * gradient * gradient
    update = new_first / bias_one / (jnp.sqrt(new_second / bias_two) + adam_eps)
    return new_first, new_second, update


def hub_kernel(scale_ref, own_ref, outer_ref, far_ref, m_ref, v_ref, mv_ref, update_ref, sum_ref):
    rows = m_ref.shape[0]
    total = own_ref[...].astype(F32) + outer_ref[...].astype(F32) + far_ref[...].astype(F32)
    sum_ref[...] = total[:rows].astype(BF16)
    gradient = total * scale_ref[0, 0]
    mv = mv_ref[...].astype(F32)
    update_ref[:rows] = moments(gradient[:rows], mv[:rows], mv[rows:])[2].astype(BF16)
    update_ref[rows:] = moments(gradient[rows:], m_ref[...], v_ref[...])[2].astype(BF16)


def hub_chunk(scale, own, outer, far, first, second, moved, start):
    rows = first.shape[0]
    width = own.shape[1]
    tile = pick(width, 1024)
    while start % tile:
        tile -= 128
    there = lambda i: (0, i)
    shifted = lambda i: (0, start // tile + i)
    two = pl.BlockSpec((2 * rows, tile), there)
    return pl.pallas_call(
        hub_kernel,
        out_shape=[
            jax.ShapeDtypeStruct((2 * rows, width), BF16),
            jax.ShapeDtypeStruct((rows, width), BF16),
        ],
        grid=(width // tile,),
        in_specs=[
            pl.BlockSpec(memory_space=pltpu.SMEM),
            two,
            two,
            two,
            pl.BlockSpec((rows, tile), shifted),
            pl.BlockSpec((rows, tile), shifted),
            pl.BlockSpec((2 * rows, tile), shifted),
        ],
        out_specs=[two, pl.BlockSpec((rows, tile), there)],
        compiler_params=params(8),
        cost_estimate=pl.CostEstimate(
            flops=40 * rows * width * 100, bytes_accessed=30 * rows * width, transcendentals=0
        ),
        name="hub",
    )(scale, own, outer, far, first, second, moved)


def settle_kernel(
    scale_ref, hub_ref, own_ref, outer_ref, far_ref, m_ref, v_ref, near_ref, across_ref, sent_ref, *rest
):
    all_ref, first_ref, second_ref = rest[-3:]
    rows = m_ref.shape[0]
    hub = hub_ref[0, 0] == 1
    total = own_ref[...].astype(F32) + outer_ref[...].astype(F32) + far_ref[...].astype(F32)
    total = jnp.where(hub, total, sent_ref[:rows].astype(F32))
    new_first, new_second, update = moments(total * scale_ref[0, 0], m_ref[...], v_ref[...])
    first_ref[...] = new_first
    second_ref[...] = new_second
    all_ref[:rows] = jnp.where(hub, near_ref[:rows], update.astype(BF16))
    all_ref[rows : 2 * rows] = jnp.where(hub, update.astype(BF16), sent_ref[rows : 2 * rows])
    all_ref[2 * rows :] = jnp.where(hub, across_ref[...], sent_ref[2 * rows :])


def settle_chunk(scale, hub, own, outer, far, first, second, near, across, sent, start, results):
    rows, full = first.shape
    width = own.shape[1]
    tile = pick(width, 1024)
    while start % tile:
        tile -= 128
    there = lambda i: (0, i)
    second_rows = lambda i: (1, i)
    shifted = lambda i: (0, start // tile + i)
    one = pl.BlockSpec((rows, tile), second_rows)
    moment = pl.BlockSpec((rows, tile), shifted)
    smem = pl.BlockSpec(memory_space=pltpu.SMEM)
    whole = [pl.BlockSpec(memory_space=pl.ANY)] * len(results)
    return pl.pallas_call(
        settle_kernel,
        out_shape=[
            jax.ShapeDtypeStruct((4 * rows, width), BF16),
            jax.ShapeDtypeStruct((rows, full), F32),
            jax.ShapeDtypeStruct((rows, full), F32),
        ],
        grid=(width // tile,),
        in_specs=[
            smem,
            smem,
            one,
            one,
            one,
            moment,
            moment,
            pl.BlockSpec((2 * rows, tile), there),
            pl.BlockSpec((2 * rows, tile), there),
            pl.BlockSpec((4 * rows, tile), there),
            *whole,
        ],
        out_specs=[pl.BlockSpec((4 * rows, tile), there), moment, moment],
        input_output_aliases={10: 1, 11: 2} if results else {},
        compiler_params=params(8),
        cost_estimate=pl.CostEstimate(
            flops=30 * rows * width * 100, bytes_accessed=40 * rows * width, transcendentals=0
        ),
        name="settle",
    )(scale, hub, own, outer, far, first, second, near, across, sent, *results)


def spread_kernel(slot_ref, basis_ref, mine_ref, other_ref, *rest):
    out_ref, updates = rest[-2:]
    blocks = slot_ref.shape[0]
    rows = 2 * mine_ref.shape[0] // blocks
    side = blocks // 2
    for n in range(blocks):
        at = slot_ref[n]
        inner = pl.multiple_of((at % side) * rows, rows)
        updates[n * rows : (n + 1) * rows, :] = jnp.where(
            at < side, mine_ref[pl.ds(inner, rows), :], other_ref[pl.ds(inner, rows), :]
        )
    out_ref[...] = jnp.dot(
        basis_ref[...], updates[...], preferred_element_type=F32
    ).astype(BF16)


def spread_chunk(slots, basis_rows, mine, other, start, full, results):
    count, rank = basis_rows.shape
    width = mine.shape[1]
    tile = pick(width, 512)
    while start % tile:
        tile -= 128
    there = lambda i, s: (0, i)
    return pl.pallas_call(
        spread_kernel,
        out_shape=jax.ShapeDtypeStruct((count, full), BF16),
        grid_spec=pltpu.PrefetchScalarGridSpec(
            num_scalar_prefetch=1,
            grid=(width // tile,),
            in_specs=[
                pl.BlockSpec((count, rank), lambda i, s: (0, 0)),
                pl.BlockSpec((rank // 2, tile), there),
                pl.BlockSpec((rank // 2, tile), there),
                *([pl.BlockSpec(memory_space=pl.ANY)] * len(results)),
            ],
            out_specs=pl.BlockSpec((count, tile), lambda i, s: (0, start // tile + i)),
            scratch_shapes=[pltpu.VMEM((rank, tile), BF16)],
        ),
        input_output_aliases={4: 0} if results else {},
        compiler_params=params(12),
        cost_estimate=pl.CostEstimate(
            flops=2 * count * rank * width,
            bytes_accessed=2 * (count * rank + rank * width + count * width),
            transcendentals=0,
        ),
        name="spread",
    )(slots, basis_rows, mine, other, *results)


def doubling(part, bits):
    count = lax.axis_size("tensor")
    for step, bit in enumerate(bits):
        got = lax.ppermute(part, "tensor", [(t, t ^ bit) for t in range(count)])
        if step == len(bits) - 1:
            return part, got
        part = (part.astype(F32) + got.astype(F32)).astype(BF16)


def local_line(activations, out_grads, basis, first_moment, second_moment, reward_codes, token_ids):
    data_count = lax.axis_size("dp")
    tensor_count = lax.axis_size("tensor")
    data_index = lax.axis_index("dp")
    tensor_index = lax.axis_index("tensor")
    chips = data_count // CORES
    chip, core = data_index // CORES, data_index % CORES
    tokens = activations.shape[0]
    full = out_grads.shape[1]
    rows = first_moment.shape[0]

    def on_chips(pairs):
        return [(a * CORES + c, b * CORES + c) for a, b in pairs for c in range(CORES)]

    inward = on_chips([(0, 1), (3, 2)])
    outward = on_chips([(1, 0), (2, 3)])
    middle = on_chips([(1, 2), (2, 1)])
    sibling = [(i, i ^ 1) for i in range(data_count)]
    hub = ((chip == 1) | (chip == 2)).astype(jnp.int32).reshape(1, 1)

    block = jnp.arange(data_count, dtype=jnp.int32)
    block_chip = block // CORES
    far = (block_chip // 2 != chip // 2).astype(jnp.int32)
    is_hub = ((block_chip == 1) | (block_chip == 2)).astype(jnp.int32)
    slots = ((block % CORES) ^ core).astype(jnp.int32) * chips + 2 * far + is_hub

    bits = [1 << b for b in range(tensor_count.bit_length() - 1)]
    half = tokens // 2
    part_a = project(slots, basis, activations, 0, half)
    part_b = project(slots, basis, activations, half, half)
    sum_a, got_a = doubling(part_a, bits)
    sum_b, got_b = doubling(part_b, bits[::-1])

    unmasked = (token_ids != pad_token).astype(F32)
    weights = unmasked * jnp.exp(reward_temp * reward_codes.astype(F32))
    normalizer = jnp.full((8, 128), jnp.sum(weights), F32)
    for b in range(data_count.bit_length() - 1):
        normalizer = normalizer + lax.ppermute(
            normalizer, "dp", [(i, i ^ (1 << b)) for i in range(data_count)]
        )
    scale = (tokens * data_count) / normalizer[:1, :1]

    left_a = (weights[None, :half] * (sum_a.astype(F32) + got_a.astype(F32))).astype(BF16)
    left_b = (weights[None, half:] * (sum_b.astype(F32) + got_b.astype(F32))).astype(BF16)

    moved = lax.ppermute(
        jnp.concatenate([first_moment, second_moment]).astype(BF16), "dp", inward
    )

    row_count = basis.shape[0] * tensor_count // data_count
    per_owner = data_count // tensor_count
    owner = data_index // per_owner
    basis_rows = lax.dynamic_slice_in_dim(basis, data_index % per_owner * row_count, row_count, 0)
    basis_rows = jnp.where(tensor_index == owner, basis_rows, jnp.zeros_like(basis_rows))

    unit = full // sum(CHUNKS)
    starts = [unit * sum(CHUNKS[:i]) for i in range(len(CHUNKS))]
    own, outer = [], []
    for start, parts in zip(starts, CHUNKS):
        keep, give = gradient_chunk(left_a, left_b, out_grads, start, unit * parts)
        own.append(keep + lax.ppermute(give, "dp", sibling))
        outer.append(lax.ppermute(own[-1], "dp", inward))

    for bit in bits:
        pairs = [
            (d * tensor_count + (d // per_owner ^ s), d * tensor_count + (d // per_owner ^ s ^ bit))
            for d in range(data_count)
            for s in range(bit)
        ]
        basis_rows = basis_rows + lax.ppermute(basis_rows, ("dp", "tensor"), pairs)

    settled, spread = (), ()
    for start, mine, came in zip(starts, own, outer):
        across = lax.ppermute(mine[2 * rows :] + came[2 * rows :], "dp", middle)
        near, total = hub_chunk(scale, mine, came, across, first_moment, second_moment, moved, start)
        beyond = lax.ppermute(near, "dp", middle)
        sent = lax.ppermute(jnp.concatenate([total, near[rows:], beyond]), "dp", outward)
        updates, *settled = settle_chunk(
            scale, hub, mine, came, across, first_moment, second_moment, near, beyond, sent, start, settled
        )
        other = lax.ppermute(updates, "dp", sibling)
        spread = (spread_chunk(slots, basis_rows, updates, other, start, full, spread),)
    return (*settled, *spread)


def solution(mesh):
    data_count, tensor_count = mesh.shape["dp"], mesh.shape["tensor"]
    line = data_count == 4 * CORES and tensor_count > 1 and tensor_count & (tensor_count - 1) == 0
    line = line and data_count % tensor_count == 0
    return jax.shard_map(
        local_line if line else local_general,
        mesh=mesh,
        in_specs=(
            P("dp", "tensor"),
            P("dp", "tensor"),
            P("tensor", None),
            P("dp", "tensor"),
            P("dp", "tensor"),
            P("dp"),
            P("dp"),
        ),
        out_specs=(P("dp", "tensor"), P("dp", "tensor"), P("dp", "tensor")),
        check_vma=False,
    )
```

```python
import functools

import jax
import jax.numpy as jnp
from jax import lax
from jax.experimental import pallas as pl
from jax.experimental.pallas import tpu as pltpu
from jax.sharding import PartitionSpec as P


ADAM_STEP = 100


pad_token = 128004
reward_temp = 0.2
beta_one = 0.9
beta_two = 0.999
adam_eps = 1e-08

bias_one = 1.0 - beta_one**ADAM_STEP
bias_two = 1.0 - beta_two**ADAM_STEP

F32, BF16 = jnp.float32, jnp.bfloat16
CORES = 2
CHUNKS = (4, 4, 4, 2)
MIB = 1 << 20


def from_root(block, axis, owner):
    block = jnp.where(lax.axis_index(axis) == owner, block, jnp.zeros_like(block))
    return lax.psum(block, axis)


def local_general(activations, out_grads, basis, first_moment, second_moment, reward_codes, token_ids):
    data_count = lax.axis_size("dp")
    tensor_count = lax.axis_size("tensor")
    partial_value = jnp.dot(activations, basis, preferred_element_type=jnp.float32)
    projected = lax.psum(partial_value.astype(jnp.bfloat16), "tensor").astype(jnp.float32)
    unmasked = (token_ids != pad_token).astype(jnp.float32)
    weights = unmasked * jnp.exp(reward_temp * reward_codes.astype(jnp.float32))
    local_total = jnp.sum(weights)
    weighted = (weights[:, None] * projected).astype(jnp.bfloat16)
    raw_grad = lax.dot_general(
        weighted, out_grads, (((0,), (0,)), ((), ())), preferred_element_type=jnp.float32
    )
    normalizer = lax.psum(local_total, "dp")
    grad_rows = lax.psum_scatter(
        raw_grad.astype(jnp.bfloat16), "dp", scatter_dimension=0, tiled=True
    ).astype(jnp.float32)
    token_count = activations.shape[0] * data_count
    gradient = grad_rows * (token_count / normalizer)
    new_first = beta_one * first_moment + (1.0 - beta_one) * gradient
    new_second = beta_two * second_moment + (1.0 - beta_two) * gradient * gradient
    update = (new_first / bias_one / (jnp.sqrt(new_second / bias_two) + adam_eps)).astype(
        jnp.bfloat16
    )
    row_count = basis.shape[0] * tensor_count // data_count
    data_index = lax.axis_index("dp")
    owner_index = data_index * tensor_count // data_count
    owner_rows = from_root(basis, "tensor", owner_index)
    offset = data_index % (data_count // tensor_count) * row_count
    basis_rows = lax.dynamic_slice_in_dim(owner_rows, offset, row_count, 0)
    summed = jnp.dot(
        basis_rows,
        lax.all_gather(update, "dp", axis=0, tiled=True),
        preferred_element_type=jnp.float32,
    )
    return (new_first, new_second, summed.astype(jnp.bfloat16))


def pick(value, width):
    best = 128
    for w in range(128, width + 1, 128):
        if value % w == 0:
            best = w
    return best


def params(limit_mib):
    return pltpu.CompilerParams(
        dimension_semantics=("arbitrary",), vmem_limit_bytes=limit_mib * MIB
    )


def project_pieces(turned, act_hbm, out_ref, act_buf, act_sem, start):
    pieces = act_sem.shape[0]
    size = act_buf.shape[0] // pieces
    copies = []
    for i in range(pieces):
        copies.append(
            pltpu.make_async_copy(
                act_hbm.at[pl.ds(start + i * size, size)],
                act_buf.at[pl.ds(i * size, size)],
                act_sem.at[i],
            )
        )
        copies[-1].start()
    yield
    for i, copy in enumerate(copies):
        copy.wait()
        out_ref[:, i * size : (i + 1) * size] = lax.dot_general(
            turned[...],
            act_buf[i * size : (i + 1) * size, :],
            (((1,), (1,)), ((), ())),
            preferred_element_type=F32,
        ).astype(out_ref.dtype)
    yield


def project_first_kernel(
    start, slot_ref, basis_hbm, act_hbm, out_ref, turned_ref, basis_buf, basis_sem, act_buf, act_sem
):
    rows = basis_buf.shape[1] // slot_ref.shape[0]
    copy = pltpu.make_async_copy(basis_hbm, basis_buf, basis_sem)
    copy.start()
    work = project_pieces(turned_ref, act_hbm, out_ref, act_buf, act_sem, start)
    next(work)
    copy.wait()
    flipped = basis_buf[...].T
    for n in range(slot_ref.shape[0]):
        at = pl.multiple_of(slot_ref[n] * rows, rows)
        turned_ref[pl.ds(at, rows), :] = flipped[n * rows : (n + 1) * rows, :]
    next(work)


def project_kernel(start, turned_ref, act_hbm, out_ref, act_buf, act_sem):
    work = project_pieces(turned_ref, act_hbm, out_ref, act_buf, act_sem, start)
    next(work)
    next(work)


def project(source, slots, activations, start, count):
    depth = activations.shape[1]
    rank = source.shape[1] if slots is not None else source.shape[0]
    hbm = pl.BlockSpec(memory_space=pltpu.HBM)
    vmem = pl.BlockSpec(memory_space=pltpu.VMEM)
    part = jax.ShapeDtypeStruct((rank, count), BF16)
    scratch = [
        pltpu.VMEM((count, depth), BF16),
        pltpu.SemaphoreType.DMA((count // pick(count, 256),)),
    ]
    estimate = pl.CostEstimate(
        flops=2 * depth * rank * count,
        bytes_accessed=2 * (depth * rank + depth * count + rank * count),
        transcendentals=0,
    )
    if slots is None:
        return pl.pallas_call(
            functools.partial(project_kernel, start),
            out_shape=part,
            in_specs=[vmem, hbm],
            out_specs=vmem,
            scratch_shapes=scratch,
            compiler_params=pltpu.CompilerParams(vmem_limit_bytes=16 * MIB),
            cost_estimate=estimate,
            name="project",
        )(source, activations)
    return pl.pallas_call(
        functools.partial(project_first_kernel, start),
        out_shape=[part, jax.ShapeDtypeStruct((rank, depth), BF16)],
        in_specs=[pl.BlockSpec(memory_space=pltpu.SMEM), hbm, hbm],
        out_specs=[vmem, vmem],
        scratch_shapes=[pltpu.VMEM((depth, rank), BF16), pltpu.SemaphoreType.DMA, *scratch],
        compiler_params=pltpu.CompilerParams(vmem_limit_bytes=16 * MIB),
        cost_estimate=estimate,
        name="project_first",
    )(slots, source, activations)


def gradient_kernel(*refs):
    *lefts, grads_ref, keep_ref, give_ref = refs
    total, at = None, 0
    for left in lefts:
        size = left.shape[1]
        term = jnp.dot(left[...], grads_ref[at : at + size, :], preferred_element_type=F32)
        total = term if total is None else total + term
        at += size
    rows = keep_ref.shape[0]
    keep_ref[...] = total[:rows].astype(BF16)
    give_ref[...] = total[rows:].astype(BF16)


def gradient_chunk(lefts, out_grads, start, width):
    rank = lefts[0].shape[0]
    tokens = out_grads.shape[0]
    tile = pick(width, 512)
    while start % tile:
        tile -= 128
    return pl.pallas_call(
        gradient_kernel,
        out_shape=[jax.ShapeDtypeStruct((rank // 2, width), BF16)] * 2,
        grid=(width // tile,),
        in_specs=[
            *(pl.BlockSpec(left.shape, lambda i: (0, 0)) for left in lefts),
            pl.BlockSpec((tokens, tile), lambda i: (0, start // tile + i)),
        ],
        out_specs=[pl.BlockSpec((rank // 2, tile), lambda i: (0, i))] * 2,
        compiler_params=params(44),
        cost_estimate=pl.CostEstimate(
            flops=2 * rank * tokens * width,
            bytes_accessed=2 * (rank * tokens + tokens * width + rank * width),
            transcendentals=0,
        ),
        name="gradient",
    )(*lefts, out_grads)


def moments(gradient, first, second):
    new_first = beta_one * first + (1.0 - beta_one) * gradient
    new_second = beta_two * second + (1.0 - beta_two) * gradient * gradient
    update = new_first / bias_one / (jnp.sqrt(new_second / bias_two) + adam_eps)
    return new_first, new_second, update


def hub_kernel(scale_ref, own_ref, outer_ref, far_ref, m_ref, v_ref, mv_ref, update_ref, sum_ref):
    rows = m_ref.shape[0]
    total = own_ref[...].astype(F32) + outer_ref[...].astype(F32) + far_ref[...].astype(F32)
    sum_ref[...] = total[:rows].astype(BF16)
    gradient = total * scale_ref[0, 0]
    mv = mv_ref[...].astype(F32)
    update_ref[:rows] = moments(gradient[:rows], mv[:rows], mv[rows:])[2].astype(BF16)
    update_ref[rows:] = moments(gradient[rows:], m_ref[...], v_ref[...])[2].astype(BF16)


def hub_chunk(scale, own, outer, far, first, second, moved, start):
    rows = first.shape[0]
    width = own.shape[1]
    tile = pick(width, 1024)
    while start % tile:
        tile -= 128
    there = lambda i: (0, i)
    shifted = lambda i: (0, start // tile + i)
    two = pl.BlockSpec((2 * rows, tile), there)
    return pl.pallas_call(
        hub_kernel,
        out_shape=[
            jax.ShapeDtypeStruct((2 * rows, width), BF16),
            jax.ShapeDtypeStruct((rows, width), BF16),
        ],
        grid=(width // tile,),
        in_specs=[
            pl.BlockSpec(memory_space=pltpu.SMEM),
            two,
            two,
            two,
            pl.BlockSpec((rows, tile), shifted),
            pl.BlockSpec((rows, tile), shifted),
            pl.BlockSpec((2 * rows, tile), shifted),
        ],
        out_specs=[two, pl.BlockSpec((rows, tile), there)],
        compiler_params=params(8),
        cost_estimate=pl.CostEstimate(
            flops=40 * rows * width * 100, bytes_accessed=30 * rows * width, transcendentals=0
        ),
        name="hub",
    )(scale, own, outer, far, first, second, moved)


def settle_kernel(
    scale_ref, hub_ref, own_ref, outer_ref, far_ref, m_ref, v_ref, near_ref, across_ref, sent_ref, *rest
):
    all_ref, first_ref, second_ref = rest[-3:]
    rows = m_ref.shape[0]
    hub = hub_ref[0, 0] == 1
    total = own_ref[...].astype(F32) + outer_ref[...].astype(F32) + far_ref[...].astype(F32)
    total = jnp.where(hub, total, sent_ref[:rows].astype(F32))
    new_first, new_second, update = moments(total * scale_ref[0, 0], m_ref[...], v_ref[...])
    first_ref[...] = new_first
    second_ref[...] = new_second
    all_ref[:rows] = jnp.where(hub, near_ref[:rows], update.astype(BF16))
    all_ref[rows : 2 * rows] = jnp.where(hub, update.astype(BF16), sent_ref[rows : 2 * rows])
    all_ref[2 * rows :] = jnp.where(hub, across_ref[...], sent_ref[2 * rows :])


def settle_chunk(scale, hub, own, outer, far, first, second, near, across, sent, start, results):
    rows, full = first.shape
    width = own.shape[1]
    tile = pick(width, 1024)
    while start % tile:
        tile -= 128
    there = lambda i: (0, i)
    second_rows = lambda i: (1, i)
    shifted = lambda i: (0, start // tile + i)
    one = pl.BlockSpec((rows, tile), second_rows)
    moment = pl.BlockSpec((rows, tile), shifted)
    smem = pl.BlockSpec(memory_space=pltpu.SMEM)
    whole = [pl.BlockSpec(memory_space=pl.ANY)] * len(results)
    return pl.pallas_call(
        settle_kernel,
        out_shape=[
            jax.ShapeDtypeStruct((4 * rows, width), BF16),
            jax.ShapeDtypeStruct((rows, full), F32),
            jax.ShapeDtypeStruct((rows, full), F32),
        ],
        grid=(width // tile,),
        in_specs=[
            smem,
            smem,
            one,
            one,
            one,
            moment,
            moment,
            pl.BlockSpec((2 * rows, tile), there),
            pl.BlockSpec((2 * rows, tile), there),
            pl.BlockSpec((4 * rows, tile), there),
            *whole,
        ],
        out_specs=[pl.BlockSpec((4 * rows, tile), there), moment, moment],
        input_output_aliases={10: 1, 11: 2} if results else {},
        compiler_params=params(8),
        cost_estimate=pl.CostEstimate(
            flops=30 * rows * width * 100, bytes_accessed=40 * rows * width, transcendentals=0
        ),
        name="settle",
    )(scale, hub, own, outer, far, first, second, near, across, sent, *results)


def spread_kernel(slot_ref, basis_ref, mine_ref, other_ref, *rest):
    out_ref, updates = rest[-2:]
    blocks = slot_ref.shape[0]
    rows = 2 * mine_ref.shape[0] // blocks
    side = blocks // 2
    for n in range(blocks):
        at = slot_ref[n]
        inner = pl.multiple_of((at % side) * rows, rows)
        updates[n * rows : (n + 1) * rows, :] = jnp.where(
            at < side, mine_ref[pl.ds(inner, rows), :], other_ref[pl.ds(inner, rows), :]
        )
    out_ref[...] = jnp.dot(
        basis_ref[...], updates[...], preferred_element_type=F32
    ).astype(BF16)


def spread_chunk(slots, basis_rows, mine, other, start, full, results):
    count, rank = basis_rows.shape
    width = mine.shape[1]
    tile = pick(width, 512)
    while start % tile:
        tile -= 128
    there = lambda i, s: (0, i)
    return pl.pallas_call(
        spread_kernel,
        out_shape=jax.ShapeDtypeStruct((count, full), BF16),
        grid_spec=pltpu.PrefetchScalarGridSpec(
            num_scalar_prefetch=1,
            grid=(width // tile,),
            in_specs=[
                pl.BlockSpec((count, rank), lambda i, s: (0, 0)),
                pl.BlockSpec((rank // 2, tile), there),
                pl.BlockSpec((rank // 2, tile), there),
                *([pl.BlockSpec(memory_space=pl.ANY)] * len(results)),
            ],
            out_specs=pl.BlockSpec((count, tile), lambda i, s: (0, start // tile + i)),
            scratch_shapes=[pltpu.VMEM((rank, tile), BF16)],
        ),
        input_output_aliases={4: 0} if results else {},
        compiler_params=params(12),
        cost_estimate=pl.CostEstimate(
            flops=2 * count * rank * width,
            bytes_accessed=2 * (count * rank + rank * width + count * width),
            transcendentals=0,
        ),
        name="spread",
    )(slots, basis_rows, mine, other, *results)


def token_pieces(tokens):
    unit = 256 if tokens % 256 == 0 else 128
    count = tokens // unit
    sizes = [(count // 4 + (i < count % 4)) * unit for i in range(4)]
    return [(sum(sizes[:i]), size) for i, size in enumerate(sizes) if size]


def local_line(activations, out_grads, basis, first_moment, second_moment, reward_codes, token_ids):
    data_count = lax.axis_size("dp")
    tensor_count = lax.axis_size("tensor")
    data_index = lax.axis_index("dp")
    tensor_index = lax.axis_index("tensor")
    chips = data_count // CORES
    chip, core = data_index // CORES, data_index % CORES
    tokens = activations.shape[0]
    full = out_grads.shape[1]
    rows = first_moment.shape[0]

    def on_chips(pairs):
        return [(a * CORES + c, b * CORES + c) for a, b in pairs for c in range(CORES)]

    inward = on_chips([(0, 1), (3, 2)])
    outward = on_chips([(1, 0), (2, 3)])
    middle = on_chips([(1, 2), (2, 1)])
    sibling = [(i, i ^ 1) for i in range(data_count)]
    hub = ((chip == 1) | (chip == 2)).astype(jnp.int32).reshape(1, 1)

    block = jnp.arange(data_count, dtype=jnp.int32)
    block_chip = block // CORES
    far = (block_chip // 2 != chip // 2).astype(jnp.int32)
    is_hub = ((block_chip == 1) | (block_chip == 2)).astype(jnp.int32)
    slots = ((block % CORES) ^ core).astype(jnp.int32) * chips + 2 * far + is_hub

    bits = [1 << b for b in range(tensor_count.bit_length() - 1)]
    parts = []
    source = basis
    for i, (start, count) in enumerate(token_pieces(tokens)):
        if i == 0:
            part, source = project(basis, slots, activations, start, count)
        else:
            part = project(source, None, activations, start, count)
        parts.append(part)
    got = [None] * len(parts)
    for step in range(len(bits)):
        for i, part in enumerate(parts):
            bit = bits[step] if i % 2 == 0 else bits[-1 - step]
            if step:
                part = parts[i] = (part.astype(F32) + got[i].astype(F32)).astype(BF16)
            pairs = [(t, t ^ bit) for t in range(tensor_count)]
            got[i] = lax.ppermute(part, "tensor", pairs)

    unmasked = (token_ids != pad_token).astype(F32)
    weights = unmasked * jnp.exp(reward_temp * reward_codes.astype(F32))
    normalizer = jnp.full((8, 128), jnp.sum(weights), F32)
    for b in range(data_count.bit_length() - 1):
        pairs = [(i, i ^ (1 << b)) for i in range(data_count)]
        normalizer = normalizer + lax.ppermute(normalizer, "dp", pairs)
    scale = (tokens * data_count) / normalizer[:1, :1]

    lefts = []
    for (start, count), part, other in zip(token_pieces(tokens), parts, got):
        total = part.astype(F32) + other.astype(F32)
        lefts.append((weights[None, start : start + count] * total).astype(BF16))

    moved = lax.ppermute(jnp.concatenate([first_moment, second_moment]).astype(BF16), "dp", inward)
    lefts, moved, scale = lax.optimization_barrier((lefts, moved, scale))

    row_count = basis.shape[0] * tensor_count // data_count
    per_owner = data_count // tensor_count
    owner = data_index // per_owner
    basis_rows = lax.dynamic_slice_in_dim(basis, data_index % per_owner * row_count, row_count, 0)
    basis_rows = jnp.where(tensor_index == owner, basis_rows, jnp.zeros_like(basis_rows))
    for bit in bits:
        pairs = [
            (d * tensor_count + (d // per_owner ^ s), d * tensor_count + (d // per_owner ^ s ^ bit))
            for d in range(data_count)
            for s in range(bit)
        ]
        basis_rows = basis_rows + lax.ppermute(basis_rows, ("dp", "tensor"), pairs)

    unit = full // sum(CHUNKS)
    starts = [unit * sum(CHUNKS[:i]) for i in range(len(CHUNKS))]
    settled, spread = (), ()
    for start, size in zip(starts, CHUNKS):
        keep, give = gradient_chunk(lefts, out_grads, start, unit * size)
        mine = keep + lax.ppermute(give, "dp", sibling)
        came = lax.ppermute(mine, "dp", inward)
        across = lax.ppermute(mine[2 * rows :] + came[2 * rows :], "dp", middle)
        near, total = hub_chunk(
            scale, mine, came, across, first_moment, second_moment, moved, start
        )
        beyond = lax.ppermute(near, "dp", middle)
        sent = lax.ppermute(jnp.concatenate([total, near[rows:], beyond]), "dp", outward)
        updates, *settled = settle_chunk(
            scale, hub, mine, came, across, first_moment, second_moment, near, beyond, sent, start, settled
        )
        other = lax.ppermute(updates, "dp", sibling)
        spread = (spread_chunk(slots, basis_rows, updates, other, start, full, spread),)
    return (*settled, *spread)


def staged(*args):
    return local_line(*args)


def solution(mesh):
    data_count, tensor_count = mesh.shape["dp"], mesh.shape["tensor"]
    line = data_count == 4 * CORES and tensor_count > 1 and tensor_count & (tensor_count - 1) == 0
    line = line and data_count % tensor_count == 0
    return jax.shard_map(
        staged if line else local_general,
        mesh=mesh,
        in_specs=(
            P("dp", "tensor"),
            P("dp", "tensor"),
            P("tensor", None),
            P("dp", "tensor"),
            P("dp", "tensor"),
            P("dp"),
            P("dp"),
        ),
        out_specs=(P("dp", "tensor"), P("dp", "tensor"), P("dp", "tensor")),
        check_vma=False,
    )
```

```python
import functools

import jax
import jax.numpy as jnp
from jax import lax
from jax.experimental import pallas as pl
from jax.experimental.pallas import tpu as pltpu
from jax.sharding import PartitionSpec as P


ADAM_STEP = 100


pad_token = 128004
reward_temp = 0.2
beta_one = 0.9
beta_two = 0.999
adam_eps = 1e-08

bias_one = 1.0 - beta_one**ADAM_STEP
bias_two = 1.0 - beta_two**ADAM_STEP

F32, BF16 = jnp.float32, jnp.bfloat16
CORES = 2
CHUNKS = (3, 4, 4, 3)
MIB = 1 << 20


def from_root(block, axis, owner):
    block = jnp.where(lax.axis_index(axis) == owner, block, jnp.zeros_like(block))
    return lax.psum(block, axis)


def local_general(activations, out_grads, basis, first_moment, second_moment, reward_codes, token_ids):
    data_count = lax.axis_size("dp")
    tensor_count = lax.axis_size("tensor")
    partial_value = jnp.dot(activations, basis, preferred_element_type=jnp.float32)
    projected = lax.psum(partial_value.astype(jnp.bfloat16), "tensor").astype(jnp.float32)
    unmasked = (token_ids != pad_token).astype(jnp.float32)
    weights = unmasked * jnp.exp(reward_temp * reward_codes.astype(jnp.float32))
    local_total = jnp.sum(weights)
    weighted = (weights[:, None] * projected).astype(jnp.bfloat16)
    raw_grad = lax.dot_general(
        weighted, out_grads, (((0,), (0,)), ((), ())), preferred_element_type=jnp.float32
    )
    normalizer = lax.psum(local_total, "dp")
    grad_rows = lax.psum_scatter(
        raw_grad.astype(jnp.bfloat16), "dp", scatter_dimension=0, tiled=True
    ).astype(jnp.float32)
    token_count = activations.shape[0] * data_count
    gradient = grad_rows * (token_count / normalizer)
    new_first = beta_one * first_moment + (1.0 - beta_one) * gradient
    new_second = beta_two * second_moment + (1.0 - beta_two) * gradient * gradient
    update = (new_first / bias_one / (jnp.sqrt(new_second / bias_two) + adam_eps)).astype(
        jnp.bfloat16
    )
    row_count = basis.shape[0] * tensor_count // data_count
    data_index = lax.axis_index("dp")
    owner_index = data_index * tensor_count // data_count
    owner_rows = from_root(basis, "tensor", owner_index)
    offset = data_index % (data_count // tensor_count) * row_count
    basis_rows = lax.dynamic_slice_in_dim(owner_rows, offset, row_count, 0)
    summed = jnp.dot(
        basis_rows,
        lax.all_gather(update, "dp", axis=0, tiled=True),
        preferred_element_type=jnp.float32,
    )
    return (new_first, new_second, summed.astype(jnp.bfloat16))


def pick(value, width):
    best = 128
    for w in range(128, width + 1, 128):
        if value % w == 0:
            best = w
    return best


def project_pieces(turned, act_hbm, out_ref, act_buf, act_sem, start):
    pieces = act_sem.shape[0]
    size = act_buf.shape[0] // pieces
    copies = []
    for i in range(pieces):
        copies.append(
            pltpu.make_async_copy(
                act_hbm.at[pl.ds(start + i * size, size)],
                act_buf.at[pl.ds(i * size, size)],
                act_sem.at[i],
            )
        )
        copies[-1].start()
    yield
    for i, copy in enumerate(copies):
        copy.wait()
        out_ref[:, i * size : (i + 1) * size] = lax.dot_general(
            turned[...],
            act_buf[i * size : (i + 1) * size, :],
            (((1,), (1,)), ((), ())),
            preferred_element_type=F32,
        ).astype(out_ref.dtype)
    yield


def project_first_kernel(
    start, slot_ref, basis_hbm, act_hbm, out_ref, turned_ref, basis_buf, basis_sem, act_buf, act_sem
):
    rows = basis_buf.shape[1] // slot_ref.shape[0]
    copy = pltpu.make_async_copy(basis_hbm, basis_buf, basis_sem)
    copy.start()
    work = project_pieces(turned_ref, act_hbm, out_ref, act_buf, act_sem, start)
    next(work)
    copy.wait()
    flipped = basis_buf[...].T
    for n in range(slot_ref.shape[0]):
        at = pl.multiple_of(slot_ref[n] * rows, rows)
        turned_ref[pl.ds(at, rows), :] = flipped[n * rows : (n + 1) * rows, :]
    next(work)


def project_kernel(start, turned_ref, act_hbm, out_ref, act_buf, act_sem):
    work = project_pieces(turned_ref, act_hbm, out_ref, act_buf, act_sem, start)
    next(work)
    next(work)


def project(source, slots, activations, start, count):
    depth = activations.shape[1]
    rank = source.shape[1] if slots is not None else source.shape[0]
    hbm = pl.BlockSpec(memory_space=pltpu.HBM)
    vmem = pl.BlockSpec(memory_space=pltpu.VMEM)
    part = jax.ShapeDtypeStruct((rank, count), BF16)
    scratch = [
        pltpu.VMEM((count, depth), BF16),
        pltpu.SemaphoreType.DMA((count // pick(count, 256),)),
    ]
    estimate = pl.CostEstimate(
        flops=2 * depth * rank * count,
        bytes_accessed=2 * (depth * rank + depth * count + rank * count),
        transcendentals=0,
    )
    if slots is None:
        return pl.pallas_call(
            functools.partial(project_kernel, start),
            out_shape=part,
            in_specs=[vmem, hbm],
            out_specs=vmem,
            scratch_shapes=scratch,
            compiler_params=pltpu.CompilerParams(vmem_limit_bytes=56 * MIB),
            cost_estimate=estimate,
            name="project",
        )(source, activations)
    return pl.pallas_call(
        functools.partial(project_first_kernel, start),
        out_shape=[part, jax.ShapeDtypeStruct((rank, depth), BF16)],
        in_specs=[pl.BlockSpec(memory_space=pltpu.SMEM), hbm, hbm],
        out_specs=[vmem, vmem],
        scratch_shapes=[pltpu.VMEM((depth, rank), BF16), pltpu.SemaphoreType.DMA, *scratch],
        compiler_params=pltpu.CompilerParams(vmem_limit_bytes=56 * MIB),
        cost_estimate=estimate,
        name="project_first",
    )(slots, source, activations)


VMEM = pl.BlockSpec(memory_space=pltpu.VMEM)
SMEM = pl.BlockSpec(memory_space=pltpu.SMEM)
HBM = pl.BlockSpec(memory_space=pltpu.HBM)


def small(limit_mib):
    return pltpu.CompilerParams(vmem_limit_bytes=limit_mib * MIB)


def load_kernel(start, source, out_ref, sem):
    parts = sem.shape[0]
    size = out_ref.shape[0] // parts
    copies = [
        pltpu.make_async_copy(
            source.at[pl.ds(start + i * size, size)], out_ref.at[pl.ds(i * size, size)], sem.at[i]
        )
        for i in range(parts)
    ]
    for copy in copies:
        copy.start()
    for copy in copies:
        copy.wait()


def load_rows(source, start, count):
    return pl.pallas_call(
        functools.partial(load_kernel, start),
        out_shape=jax.ShapeDtypeStruct((count, source.shape[1]), source.dtype),
        in_specs=[HBM],
        out_specs=VMEM,
        scratch_shapes=[pltpu.SemaphoreType.DMA((count // 128,))],
        compiler_params=small(16),
        cost_estimate=pl.CostEstimate(
            flops=count * 10**6, bytes_accessed=4 * count * source.shape[1], transcendentals=0
        ),
        name="load",
    )(source)


def gradient_kernel(start, tile, pieces, *refs):
    lefts, grads = refs[:pieces], refs[pieces:-2]
    keep_ref, give_ref = refs[-2:]
    rows, width = keep_ref.shape

    def body(i, _):
        at = pl.multiple_of(i * tile, tile)
        total, piece, row = None, 0, 0
        for left in lefts:
            count = left.shape[1]
            if row == grads[piece].shape[0]:
                piece, row = piece + 1, 0
            term = jnp.dot(
                left[...],
                grads[piece][row : row + count, pl.ds(start + at, tile)],
                preferred_element_type=F32,
            )
            row += count
            total = term if total is None else total + term
        keep_ref[:, pl.ds(at, tile)] = total[:rows].astype(BF16)
        give_ref[:, pl.ds(at, tile)] = total[rows:].astype(BF16)
        return 0

    lax.fori_loop(0, width // tile, body, 0)


def gradient_chunk(lefts, grads, start, width):
    rank = lefts[0].shape[0]
    tokens = sum(piece.shape[0] for piece in grads)
    return pl.pallas_call(
        functools.partial(gradient_kernel, start, pick(width, 512), len(lefts)),
        out_shape=[jax.ShapeDtypeStruct((rank // 2, width), BF16)] * 2,
        in_specs=[VMEM] * (len(lefts) + len(grads)),
        out_specs=[VMEM, VMEM],
        compiler_params=small(4),
        cost_estimate=pl.CostEstimate(
            flops=2 * rank * tokens * width, bytes_accessed=4 * rank * width, transcendentals=0
        ),
        name="gradient",
    )(*lefts, *grads)


def moments(gradient, first, second):
    new_first = beta_one * first + (1.0 - beta_one) * gradient
    new_second = beta_two * second + (1.0 - beta_two) * gradient * gradient
    update = new_first / bias_one / (jnp.sqrt(new_second / bias_two) + adam_eps)
    return new_first, new_second, update


def hub_kernel(
    start, scale_ref, own_ref, came_ref, far_ref, m_ref, v_ref, mv_ref, near_ref, sum_ref, mine_ref
):
    rows, width = mine_ref.shape
    total = own_ref[: 2 * rows].astype(F32) + came_ref[: 2 * rows].astype(F32)
    total = total + far_ref[...].astype(F32)
    sum_ref[...] = total[:rows].astype(BF16)
    mine_ref[...] = total[rows:]
    gradient = total * scale_ref[0, 0]
    cols = slice(start, start + width)
    mv = mv_ref[:, cols].astype(F32)
    near_ref[:rows] = moments(gradient[:rows], mv[:rows], mv[rows:])[2].astype(BF16)
    near_ref[rows:] = moments(gradient[rows:], m_ref[:, cols], v_ref[:, cols])[2].astype(BF16)


def hub_chunk(scale, own, came, far, first, second, moved, start):
    rows, width = first.shape[0], own.shape[1]
    return pl.pallas_call(
        functools.partial(hub_kernel, start),
        out_shape=[
            jax.ShapeDtypeStruct((2 * rows, width), BF16),
            jax.ShapeDtypeStruct((rows, width), BF16),
            jax.ShapeDtypeStruct((rows, width), F32),
        ],
        in_specs=[SMEM] + [VMEM] * 6,
        out_specs=[VMEM] * 3,
        compiler_params=small(4),
        cost_estimate=pl.CostEstimate(
            flops=4000 * rows * width, bytes_accessed=30 * rows * width, transcendentals=0
        ),
        name="hub",
    )(scale, own, came, far, first, second, moved)


def settle_kernel(
    start, scale_ref, hub_ref, mine_ref, m_ref, v_ref, near_ref, across_ref, sent_ref, *rest
):
    all_ref, first_out, second_out, first_buf, second_buf, sem = rest[-6:]
    rows, width = mine_ref.shape
    cols = slice(start, start + width)
    hub = hub_ref[0, 0] == 1
    total = jnp.where(hub, mine_ref[...], sent_ref[:rows].astype(F32))
    new_first, new_second, update = moments(
        total * scale_ref[0, 0], m_ref[:, cols], v_ref[:, cols]
    )
    first_buf[...] = new_first
    second_buf[...] = new_second
    copies = [
        pltpu.make_async_copy(first_buf, first_out.at[:, pl.ds(start, width)], sem.at[0]),
        pltpu.make_async_copy(second_buf, second_out.at[:, pl.ds(start, width)], sem.at[1]),
    ]
    for copy in copies:
        copy.start()
    all_ref[:rows] = jnp.where(hub, near_ref[:rows], update.astype(BF16))
    all_ref[rows : 2 * rows] = jnp.where(hub, update.astype(BF16), sent_ref[rows : 2 * rows])
    all_ref[2 * rows :] = jnp.where(hub, across_ref[...], sent_ref[2 * rows :])
    for copy in copies:
        copy.wait()


def settle_chunk(scale, hub, mine, first, second, near, across, sent, start, results):
    rows, full = first.shape
    width = mine.shape[1]
    return pl.pallas_call(
        functools.partial(settle_kernel, start),
        out_shape=[
            jax.ShapeDtypeStruct((4 * rows, width), BF16),
            jax.ShapeDtypeStruct((rows, full), F32),
            jax.ShapeDtypeStruct((rows, full), F32),
        ],
        in_specs=[SMEM, SMEM] + [VMEM] * 6 + [HBM] * len(results),
        out_specs=[VMEM, HBM, HBM],
        input_output_aliases={8: 1, 9: 2} if results else {},
        scratch_shapes=[
            pltpu.VMEM((rows, width), F32),
            pltpu.VMEM((rows, width), F32),
            pltpu.SemaphoreType.DMA((2,)),
        ],
        compiler_params=small(4),
        cost_estimate=pl.CostEstimate(
            flops=4000 * rows * width, bytes_accessed=40 * rows * width, transcendentals=0
        ),
        name="settle",
    )(scale, hub, mine, first, second, near, across, sent, *results)


def spread_kernel(start, slot_ref, basis_ref, mine_ref, other_ref, *rest):
    out_ref, updates, buf, sem = rest[-4:]
    blocks = slot_ref.shape[0]
    width = mine_ref.shape[1]
    rows = 2 * mine_ref.shape[0] // blocks
    side = blocks // 2
    for n in range(blocks):
        at = slot_ref[n]
        inner = pl.multiple_of((at % side) * rows, rows)
        updates[n * rows : (n + 1) * rows, :] = jnp.where(
            at < side, mine_ref[pl.ds(inner, rows), :], other_ref[pl.ds(inner, rows), :]
        )
    steps = sem.shape[0]
    size = basis_ref.shape[0] // steps
    copies = []
    for i in range(steps):
        part = pl.ds(i * size, size)
        buf[part, :] = jnp.dot(
            basis_ref[part, :], updates[...], preferred_element_type=F32
        ).astype(BF16)
        copies.append(
            pltpu.make_async_copy(
                buf.at[part], out_ref.at[part, pl.ds(start, width)], sem.at[i]
            )
        )
        copies[-1].start()
    for copy in copies:
        copy.wait()


def spread_chunk(slots, basis_rows, mine, other, start, full, results):
    count, rank = basis_rows.shape
    width = mine.shape[1]
    return pl.pallas_call(
        functools.partial(spread_kernel, start),
        out_shape=jax.ShapeDtypeStruct((count, full), BF16),
        in_specs=[SMEM] + [VMEM] * 3 + [HBM] * len(results),
        out_specs=HBM,
        scratch_shapes=[
            pltpu.VMEM((rank, width), BF16),
            pltpu.VMEM((count, width), BF16),
            pltpu.SemaphoreType.DMA((4 if count % 64 == 0 else 1,)),
        ],
        input_output_aliases={4: 0} if results else {},
        compiler_params=small(9),
        cost_estimate=pl.CostEstimate(
            flops=2 * count * rank * width,
            bytes_accessed=2 * (count * rank + rank * width + count * width),
            transcendentals=0,
        ),
        name="spread",
    )(slots, basis_rows, mine, other, *results)


def token_pieces(tokens):
    unit = 256 if tokens % 256 == 0 else 128
    count = tokens // unit
    sizes = [(count // 4 + (i < count % 4)) * unit for i in range(4)]
    return [(sum(sizes[:i]), size) for i, size in enumerate(sizes) if size]


def local_line(activations, out_grads, basis, first_moment, second_moment, reward_codes, token_ids):
    data_count = lax.axis_size("dp")
    tensor_count = lax.axis_size("tensor")
    data_index = lax.axis_index("dp")
    tensor_index = lax.axis_index("tensor")
    chips = data_count // CORES
    chip, core = data_index // CORES, data_index % CORES
    tokens = activations.shape[0]
    full = out_grads.shape[1]
    rows = first_moment.shape[0]

    def on_chips(pairs):
        return [(a * CORES + c, b * CORES + c) for a, b in pairs for c in range(CORES)]

    inward = on_chips([(0, 1), (3, 2)])
    outward = on_chips([(1, 0), (2, 3)])
    middle = on_chips([(1, 2), (2, 1)])
    sibling = [(i, i ^ 1) for i in range(data_count)]
    hub = ((chip == 1) | (chip == 2)).astype(jnp.int32).reshape(1, 1)

    block = jnp.arange(data_count, dtype=jnp.int32)
    block_chip = block // CORES
    far = (block_chip // 2 != chip // 2).astype(jnp.int32)
    is_hub = ((block_chip == 1) | (block_chip == 2)).astype(jnp.int32)
    slots = ((block % CORES) ^ core).astype(jnp.int32) * chips + 2 * far + is_hub

    row_count = basis.shape[0] * tensor_count // data_count
    per_owner = data_count // tensor_count
    owner = data_index // per_owner
    basis_rows = lax.dynamic_slice_in_dim(basis, data_index % per_owner * row_count, row_count, 0)
    basis_rows = jnp.where(tensor_index == owner, basis_rows, jnp.zeros_like(basis_rows))
    bits = [1 << b for b in range(tensor_count.bit_length() - 1)]
    parts = []
    source = basis
    for i, (start, count) in enumerate(token_pieces(tokens)):
        if i == 0:
            part, source = project(basis, slots, activations, start, count)
        else:
            part = project(source, None, activations, start, count)
        parts.append(part)
    got = [None] * len(parts)
    for step in range(len(bits)):
        for i, part in enumerate(parts):
            bit = bits[step] if i % 2 == 0 else bits[-1 - step]
            if step:
                part = parts[i] = (part.astype(F32) + got[i].astype(F32)).astype(BF16)
            pairs = [(t, t ^ bit) for t in range(tensor_count)]
            got[i] = lax.ppermute(part, "tensor", pairs)

    unmasked = (token_ids != pad_token).astype(F32)
    weights = unmasked * jnp.exp(reward_temp * reward_codes.astype(F32))
    normalizer = jnp.full((8, 128), jnp.sum(weights), F32)
    for b in range(data_count.bit_length() - 1):
        pairs = [(i, i ^ (1 << b)) for i in range(data_count)]
        normalizer = normalizer + lax.ppermute(normalizer, "dp", pairs)
    scale = (tokens * data_count) / normalizer[:1, :1]

    lefts = []
    for (start, count), part, other in zip(token_pieces(tokens), parts, got):
        total = part.astype(F32) + other.astype(F32)
        lefts.append((weights[None, start : start + count] * total).astype(BF16))

    moved = lax.ppermute(jnp.concatenate([first_moment, second_moment]).astype(BF16), "dp", inward)
    lefts, moved, scale = lax.optimization_barrier((lefts, moved, scale))
    out_grads, basis_rows, hub, slots = lax.optimization_barrier(
        (out_grads, basis_rows, hub, slots)
    )
    grads = []
    spans = token_pieces(tokens)
    cut = spans[2][0]
    for start, count in ((0, cut), (cut, tokens - cut)):
        grads.append(load_rows(out_grads, start, count))

    for bit in bits:
        pairs = [
            (d * tensor_count + (d // per_owner ^ s), d * tensor_count + (d // per_owner ^ s ^ bit))
            for d in range(data_count)
            for s in range(bit)
        ]
        basis_rows = basis_rows + lax.ppermute(basis_rows, ("dp", "tensor"), pairs)

    unit = full // sum(CHUNKS)
    starts = [unit * sum(CHUNKS[:i]) for i in range(len(CHUNKS))]
    settled, spread = (), ()
    for start, size in zip(starts, CHUNKS):
        keep, give = gradient_chunk(lefts, grads, start, unit * size)
        mine = keep + lax.ppermute(give, "dp", sibling)
        came = lax.ppermute(mine, "dp", inward)
        across = lax.ppermute(mine[2 * rows :] + came[2 * rows :], "dp", middle)
        near, total, held = hub_chunk(
            scale, mine, came, across, first_moment, second_moment, moved, start
        )
        beyond = lax.ppermute(near, "dp", middle)
        sent = lax.ppermute(jnp.concatenate([total, near[rows:], beyond]), "dp", outward)
        updates, *settled = settle_chunk(
            scale, hub, held, first_moment, second_moment, near, beyond, sent, start, settled
        )
        other = lax.ppermute(updates, "dp", sibling)
        spread = (spread_chunk(slots, basis_rows, updates, other, start, full, spread),)
    return (*settled, *spread)


def staged(*args):
    return local_line(*args)


def solution(mesh):
    data_count, tensor_count = mesh.shape["dp"], mesh.shape["tensor"]
    line = data_count == 4 * CORES and tensor_count > 1 and tensor_count & (tensor_count - 1) == 0
    line = line and data_count % tensor_count == 0
    return jax.shard_map(
        staged if line else local_general,
        mesh=mesh,
        in_specs=(
            P("dp", "tensor"),
            P("dp", "tensor"),
            P("tensor", None),
            P("dp", "tensor"),
            P("dp", "tensor"),
            P("dp"),
            P("dp"),
        ),
        out_specs=(P("dp", "tensor"), P("dp", "tensor"), P("dp", "tensor")),
        check_vma=False,
    )
```

```python
import functools

import jax
import jax.numpy as jnp
from jax import lax
from jax.experimental import pallas as pl
from jax.experimental.pallas import tpu as pltpu
from jax.sharding import PartitionSpec as P


ADAM_STEP = 100


pad_token = 128004
reward_temp = 0.2
beta_one = 0.9
beta_two = 0.999
adam_eps = 1e-08

bias_one = 1.0 - beta_one**ADAM_STEP
bias_two = 1.0 - beta_two**ADAM_STEP

F32, BF16 = jnp.float32, jnp.bfloat16
CORES = 2
CHUNKS = (3, 4, 4, 3)
MIB = 1 << 20

VMEM = pl.BlockSpec(memory_space=pltpu.VMEM)
SMEM = pl.BlockSpec(memory_space=pltpu.SMEM)
HBM = pl.BlockSpec(memory_space=pltpu.HBM)


def from_root(block, axis, owner):
    block = jnp.where(lax.axis_index(axis) == owner, block, jnp.zeros_like(block))
    return lax.psum(block, axis)


def local_general(activations, out_grads, basis, first_moment, second_moment, reward_codes, token_ids):
    data_count = lax.axis_size("dp")
    tensor_count = lax.axis_size("tensor")
    partial_value = jnp.dot(activations, basis, preferred_element_type=jnp.float32)
    projected = lax.psum(partial_value.astype(jnp.bfloat16), "tensor").astype(jnp.float32)
    unmasked = (token_ids != pad_token).astype(jnp.float32)
    weights = unmasked * jnp.exp(reward_temp * reward_codes.astype(jnp.float32))
    local_total = jnp.sum(weights)
    weighted = (weights[:, None] * projected).astype(jnp.bfloat16)
    raw_grad = lax.dot_general(
        weighted, out_grads, (((0,), (0,)), ((), ())), preferred_element_type=jnp.float32
    )
    normalizer = lax.psum(local_total, "dp")
    grad_rows = lax.psum_scatter(
        raw_grad.astype(jnp.bfloat16), "dp", scatter_dimension=0, tiled=True
    ).astype(jnp.float32)
    token_count = activations.shape[0] * data_count
    gradient = grad_rows * (token_count / normalizer)
    new_first = beta_one * first_moment + (1.0 - beta_one) * gradient
    new_second = beta_two * second_moment + (1.0 - beta_two) * gradient * gradient
    update = (new_first / bias_one / (jnp.sqrt(new_second / bias_two) + adam_eps)).astype(
        jnp.bfloat16
    )
    row_count = basis.shape[0] * tensor_count // data_count
    data_index = lax.axis_index("dp")
    owner_index = data_index * tensor_count // data_count
    owner_rows = from_root(basis, "tensor", owner_index)
    offset = data_index % (data_count // tensor_count) * row_count
    basis_rows = lax.dynamic_slice_in_dim(owner_rows, offset, row_count, 0)
    summed = jnp.dot(
        basis_rows,
        lax.all_gather(update, "dp", axis=0, tiled=True),
        preferred_element_type=jnp.float32,
    )
    return (new_first, new_second, summed.astype(jnp.bfloat16))


def pick(value, width):
    best = 128
    for w in range(128, width + 1, 128):
        if value % w == 0:
            best = w
    return best


def project_kernel(slot_ref, basis_hbm, act_hbm, *refs):
    *outs, turned, basis_buf, basis_sem, act_buf, act_sem = refs
    rows = basis_buf.shape[1] // slot_ref.shape[0]
    pieces = act_sem.shape[0]
    size = act_buf.shape[0] // pieces
    copy = pltpu.make_async_copy(basis_hbm, basis_buf, basis_sem)
    copy.start()
    copies = []
    for i in range(pieces):
        part = pl.ds(i * size, size)
        copies.append(pltpu.make_async_copy(act_hbm.at[part], act_buf.at[part], act_sem.at[i]))
        copies[-1].start()
    copy.wait()
    flipped = basis_buf[...].T
    for n in range(slot_ref.shape[0]):
        at = pl.multiple_of(slot_ref[n] * rows, rows)
        turned[pl.ds(at, rows), :] = flipped[n * rows : (n + 1) * rows, :]
    i = 0
    for out_ref in outs:
        for at in range(0, out_ref.shape[1], size):
            copies[i].wait()
            out_ref[:, at : at + size] = lax.dot_general(
                turned[...],
                act_buf[i * size : (i + 1) * size, :],
                (((1,), (1,)), ((), ())),
                preferred_element_type=F32,
            ).astype(out_ref.dtype)
            i += 1


def project(slots, basis, activations, spans):
    tokens, depth = activations.shape
    rank = basis.shape[1]
    size = 256 if all(count % 256 == 0 for _, count in spans) else 128
    return pl.pallas_call(
        project_kernel,
        out_shape=[jax.ShapeDtypeStruct((rank, count), BF16) for _, count in spans],
        in_specs=[SMEM, HBM, HBM],
        out_specs=[VMEM] * len(spans),
        scratch_shapes=[
            pltpu.VMEM((rank, depth), BF16),
            pltpu.VMEM((depth, rank), BF16),
            pltpu.SemaphoreType.DMA,
            pltpu.VMEM((tokens, depth), BF16),
            pltpu.SemaphoreType.DMA((tokens // size,)),
        ],
        compiler_params=pltpu.CompilerParams(vmem_limit_bytes=52 * MIB),
        cost_estimate=pl.CostEstimate(
            flops=2 * depth * rank * tokens,
            bytes_accessed=2 * (depth * rank + depth * tokens + rank * tokens),
            transcendentals=0,
        ),
        name="project",
    )(slots, basis, activations)


def small(limit_mib):
    return pltpu.CompilerParams(vmem_limit_bytes=limit_mib * MIB)


def load_kernel(start, source, out_ref, sem):
    parts = sem.shape[0]
    size = out_ref.shape[0] // parts
    copies = [
        pltpu.make_async_copy(
            source.at[pl.ds(start + i * size, size)], out_ref.at[pl.ds(i * size, size)], sem.at[i]
        )
        for i in range(parts)
    ]
    for copy in copies:
        copy.start()
    for copy in copies:
        copy.wait()


def load_rows(source, start, count):
    return pl.pallas_call(
        functools.partial(load_kernel, start),
        out_shape=jax.ShapeDtypeStruct((count, source.shape[1]), source.dtype),
        in_specs=[HBM],
        out_specs=VMEM,
        scratch_shapes=[pltpu.SemaphoreType.DMA((count // 128,))],
        compiler_params=small(16),
        cost_estimate=pl.CostEstimate(
            flops=count * 10**6, bytes_accessed=4 * count * source.shape[1], transcendentals=0
        ),
        name="load",
    )(source)


def gradient_kernel(start, tile, pieces, *refs):
    lefts, grads = refs[:pieces], refs[pieces:-2]
    keep_ref, give_ref = refs[-2:]
    rows, width = keep_ref.shape

    def body(i, _):
        at = pl.multiple_of(i * tile, tile)
        total, piece, row = None, 0, 0
        for left in lefts:
            count = left.shape[1]
            if row == grads[piece].shape[0]:
                piece, row = piece + 1, 0
            term = jnp.dot(
                left[...],
                grads[piece][row : row + count, pl.ds(start + at, tile)],
                preferred_element_type=F32,
            )
            row += count
            total = term if total is None else total + term
        keep_ref[:, pl.ds(at, tile)] = total[:rows].astype(BF16)
        give_ref[:, pl.ds(at, tile)] = total[rows:].astype(BF16)
        return 0

    lax.fori_loop(0, width // tile, body, 0)


def gradient_chunk(lefts, grads, start, width):
    rank = lefts[0].shape[0]
    tokens = sum(piece.shape[0] for piece in grads)
    return pl.pallas_call(
        functools.partial(gradient_kernel, start, pick(width, 512), len(lefts)),
        out_shape=[jax.ShapeDtypeStruct((rank // 2, width), BF16)] * 2,
        in_specs=[VMEM] * (len(lefts) + len(grads)),
        out_specs=[VMEM, VMEM],
        compiler_params=small(4),
        cost_estimate=pl.CostEstimate(
            flops=2 * rank * tokens * width, bytes_accessed=4 * rank * width, transcendentals=0
        ),
        name="gradient",
    )(*lefts, *grads)


def moments(gradient, first, second):
    new_first = beta_one * first + (1.0 - beta_one) * gradient
    new_second = beta_two * second + (1.0 - beta_two) * gradient * gradient
    update = new_first / bias_one / (jnp.sqrt(new_second / bias_two) + adam_eps)
    return new_first, new_second, update


def hub_kernel(
    start, scale_ref, own_ref, came_ref, far_ref, m_ref, v_ref, mv_ref, near_ref, out_ref, mine_ref
):
    rows, width = mine_ref.shape
    total = own_ref[: 2 * rows].astype(F32) + came_ref[: 2 * rows].astype(F32)
    total = total + far_ref[...].astype(F32)
    out_ref[:rows] = total[:rows].astype(BF16)
    mine_ref[...] = total[rows:]
    gradient = total * scale_ref[0, 0]
    cols = slice(start, start + width)
    mv = mv_ref[:, cols].astype(F32)
    near_ref[:rows] = moments(gradient[:rows], mv[:rows], mv[rows:])[2].astype(BF16)
    update = moments(gradient[rows:], m_ref[:, cols], v_ref[:, cols])[2].astype(BF16)
    near_ref[rows:] = update
    out_ref[rows:] = update


def hub_chunk(scale, own, came, far, first, second, moved, start):
    rows, width = first.shape[0], own.shape[1]
    return pl.pallas_call(
        functools.partial(hub_kernel, start),
        out_shape=[
            jax.ShapeDtypeStruct((2 * rows, width), BF16),
            jax.ShapeDtypeStruct((2 * rows, width), BF16),
            jax.ShapeDtypeStruct((rows, width), F32),
        ],
        in_specs=[SMEM] + [VMEM] * 6,
        out_specs=[VMEM] * 3,
        compiler_params=small(4),
        cost_estimate=pl.CostEstimate(
            flops=4000 * rows * width, bytes_accessed=30 * rows * width, transcendentals=0
        ),
        name="hub",
    )(scale, own, came, far, first, second, moved)


def settle_kernel(
    start, scale_ref, hub_ref, mine_ref, m_ref, v_ref, near_ref, across_ref, sent_ref, more_ref, *rest
):
    all_ref, first_out, second_out, first_buf, second_buf, sem = rest[-6:]
    rows, width = mine_ref.shape
    cols = slice(start, start + width)
    hub = hub_ref[0, 0] == 1
    total = jnp.where(hub, mine_ref[...], sent_ref[:rows].astype(F32))
    new_first, new_second, update = moments(
        total * scale_ref[0, 0], m_ref[:, cols], v_ref[:, cols]
    )
    first_buf[...] = new_first
    second_buf[...] = new_second
    copies = [
        pltpu.make_async_copy(first_buf, first_out.at[:, pl.ds(start, width)], sem.at[0]),
        pltpu.make_async_copy(second_buf, second_out.at[:, pl.ds(start, width)], sem.at[1]),
    ]
    for copy in copies:
        copy.start()
    all_ref[:rows] = jnp.where(hub, near_ref[:rows], update.astype(BF16))
    all_ref[rows : 2 * rows] = jnp.where(hub, update.astype(BF16), sent_ref[rows : 2 * rows])
    all_ref[2 * rows :] = jnp.where(hub, across_ref[...], more_ref[...])
    for copy in copies:
        copy.wait()


def settle_chunk(scale, hub, mine, first, second, near, across, sent, more, start, results):
    rows, full = first.shape
    width = mine.shape[1]
    return pl.pallas_call(
        functools.partial(settle_kernel, start),
        out_shape=[
            jax.ShapeDtypeStruct((4 * rows, width), BF16),
            jax.ShapeDtypeStruct((rows, full), F32),
            jax.ShapeDtypeStruct((rows, full), F32),
        ],
        in_specs=[SMEM, SMEM] + [VMEM] * 7 + [HBM] * len(results),
        out_specs=[VMEM, HBM, HBM],
        input_output_aliases={9: 1, 10: 2} if results else {},
        scratch_shapes=[
            pltpu.VMEM((rows, width), F32),
            pltpu.VMEM((rows, width), F32),
            pltpu.SemaphoreType.DMA((2,)),
        ],
        compiler_params=small(4),
        cost_estimate=pl.CostEstimate(
            flops=4000 * rows * width, bytes_accessed=40 * rows * width, transcendentals=0
        ),
        name="settle",
    )(scale, hub, mine, first, second, near, across, sent, more, *results)


def spread_kernel(start, slot_ref, basis_ref, mine_ref, other_ref, *rest):
    out_ref, updates, buf, sem = rest[-4:]
    blocks = slot_ref.shape[0]
    width = mine_ref.shape[1]
    rows = 2 * mine_ref.shape[0] // blocks
    side = blocks // 2
    for n in range(blocks):
        at = slot_ref[n]
        inner = pl.multiple_of((at % side) * rows, rows)
        updates[n * rows : (n + 1) * rows, :] = jnp.where(
            at < side, mine_ref[pl.ds(inner, rows), :], other_ref[pl.ds(inner, rows), :]
        )
    steps = sem.shape[0]
    size = basis_ref.shape[0] // steps
    copies = []
    for i in range(steps):
        part = pl.ds(i * size, size)
        buf[part, :] = jnp.dot(
            basis_ref[part, :], updates[...], preferred_element_type=F32
        ).astype(BF16)
        copies.append(
            pltpu.make_async_copy(
                buf.at[part], out_ref.at[part, pl.ds(start, width)], sem.at[i]
            )
        )
        copies[-1].start()
    for copy in copies:
        copy.wait()


def spread_chunk(slots, basis_rows, mine, other, start, full, results):
    count, rank = basis_rows.shape
    width = mine.shape[1]
    return pl.pallas_call(
        functools.partial(spread_kernel, start),
        out_shape=jax.ShapeDtypeStruct((count, full), BF16),
        in_specs=[SMEM] + [VMEM] * 3 + [HBM] * len(results),
        out_specs=HBM,
        scratch_shapes=[
            pltpu.VMEM((rank, width), BF16),
            pltpu.VMEM((count, width), BF16),
            pltpu.SemaphoreType.DMA((4 if count % 64 == 0 else 1,)),
        ],
        input_output_aliases={4: 0} if results else {},
        compiler_params=small(9),
        cost_estimate=pl.CostEstimate(
            flops=2 * count * rank * width,
            bytes_accessed=2 * (count * rank + rank * width + count * width),
            transcendentals=0,
        ),
        name="spread",
    )(slots, basis_rows, mine, other, *results)


def token_pieces(tokens):
    unit = 256 if tokens % 256 == 0 else 128
    count = tokens // unit
    sizes = [(count // 4 + (i < count % 4)) * unit for i in range(4)]
    return [(sum(sizes[:i]), size) for i, size in enumerate(sizes) if size]


def local_line(activations, out_grads, basis, first_moment, second_moment, reward_codes, token_ids):
    data_count = lax.axis_size("dp")
    tensor_count = lax.axis_size("tensor")
    data_index = lax.axis_index("dp")
    tensor_index = lax.axis_index("tensor")
    chips = data_count // CORES
    chip, core = data_index // CORES, data_index % CORES
    tokens = activations.shape[0]
    full = out_grads.shape[1]
    rows = first_moment.shape[0]

    def on_chips(pairs):
        return [(a * CORES + c, b * CORES + c) for a, b in pairs for c in range(CORES)]

    inward = on_chips([(0, 1), (3, 2)])
    outward = on_chips([(1, 0), (2, 3)])
    middle = on_chips([(1, 2), (2, 1)])
    sibling = [(i, i ^ 1) for i in range(data_count)]
    hub = ((chip == 1) | (chip == 2)).astype(jnp.int32).reshape(1, 1)

    block = jnp.arange(data_count, dtype=jnp.int32)
    block_chip = block // CORES
    far = (block_chip // 2 != chip // 2).astype(jnp.int32)
    is_hub = ((block_chip == 1) | (block_chip == 2)).astype(jnp.int32)
    slots = ((block % CORES) ^ core).astype(jnp.int32) * chips + 2 * far + is_hub

    row_count = basis.shape[0] * tensor_count // data_count
    per_owner = data_count // tensor_count
    owner = data_index // per_owner
    basis_rows = lax.dynamic_slice_in_dim(basis, data_index % per_owner * row_count, row_count, 0)
    basis_rows = jnp.where(tensor_index == owner, basis_rows, jnp.zeros_like(basis_rows))
    bits = [1 << b for b in range(tensor_count.bit_length() - 1)]
    parts = list(project(slots, basis, activations, token_pieces(tokens)))
    got = [None] * len(parts)
    for step in range(len(bits)):
        for i, part in enumerate(parts):
            bit = bits[step] if i % 2 == 0 else bits[-1 - step]
            if step:
                part = parts[i] = (part.astype(F32) + got[i].astype(F32)).astype(BF16)
            pairs = [(t, t ^ bit) for t in range(tensor_count)]
            got[i] = lax.ppermute(part, "tensor", pairs)

    unmasked = (token_ids != pad_token).astype(F32)
    weights = unmasked * jnp.exp(reward_temp * reward_codes.astype(F32))
    normalizer = jnp.full((8, 128), jnp.sum(weights), F32)
    for b in range(data_count.bit_length() - 1):
        pairs = [(i, i ^ (1 << b)) for i in range(data_count)]
        normalizer = normalizer + lax.ppermute(normalizer, "dp", pairs)
    scale = (tokens * data_count) / normalizer[:1, :1]

    lefts = []
    for (start, count), part, other in zip(token_pieces(tokens), parts, got):
        total = part.astype(F32) + other.astype(F32)
        lefts.append((weights[None, start : start + count] * total).astype(BF16))

    moved = lax.ppermute(jnp.concatenate([first_moment, second_moment]).astype(BF16), "dp", inward)
    lefts, moved, scale = lax.optimization_barrier((lefts, moved, scale))
    out_grads, basis_rows, hub, slots = lax.optimization_barrier(
        (out_grads, basis_rows, hub, slots)
    )
    grads = []
    spans = token_pieces(tokens)
    cut = spans[2][0]
    for start, count in ((0, cut), (cut, tokens - cut)):
        grads.append(load_rows(out_grads, start, count))

    for bit in bits:
        pairs = [
            (d * tensor_count + (d // per_owner ^ s), d * tensor_count + (d // per_owner ^ s ^ bit))
            for d in range(data_count)
            for s in range(bit)
        ]
        basis_rows = basis_rows + lax.ppermute(basis_rows, ("dp", "tensor"), pairs)

    unit = full // sum(CHUNKS)
    starts = [unit * sum(CHUNKS[:i]) for i in range(len(CHUNKS))]
    settled, spread = (), ()
    for start, size in zip(starts, CHUNKS):
        keep, give = gradient_chunk(lefts, grads, start, unit * size)
        mine = keep + lax.ppermute(give, "dp", sibling)
        came = lax.ppermute(mine, "dp", inward)
        across = lax.ppermute(mine[2 * rows :] + came[2 * rows :], "dp", middle)
        near, ready, held = hub_chunk(
            scale, mine, came, across, first_moment, second_moment, moved, start
        )
        beyond = lax.ppermute(near, "dp", middle)
        sent = lax.ppermute(ready, "dp", outward)
        more = lax.ppermute(beyond, "dp", outward)
        updates, *settled = settle_chunk(
            scale, hub, held, first_moment, second_moment, near, beyond, sent, more, start, settled
        )
        other = lax.ppermute(updates, "dp", sibling)
        spread = (spread_chunk(slots, basis_rows, updates, other, start, full, spread),)
    return (*settled, *spread)


def staged(*args):
    return local_line(*args)


def solution(mesh):
    data_count, tensor_count = mesh.shape["dp"], mesh.shape["tensor"]
    line = data_count == 4 * CORES and tensor_count > 1 and tensor_count & (tensor_count - 1) == 0
    line = line and data_count % tensor_count == 0
    return jax.shard_map(
        staged if line else local_general,
        mesh=mesh,
        in_specs=(
            P("dp", "tensor"),
            P("dp", "tensor"),
            P("tensor", None),
            P("dp", "tensor"),
            P("dp", "tensor"),
            P("dp"),
            P("dp"),
        ),
        out_specs=(P("dp", "tensor"), P("dp", "tensor"), P("dp", "tensor")),
        check_vma=False,
    )
```

```python
import functools

import jax
import jax.numpy as jnp
from jax import lax
from jax.experimental import pallas as pl
from jax.experimental.pallas import tpu as pltpu
from jax.sharding import PartitionSpec as P


ADAM_STEP = 100


pad_token = 128004
reward_temp = 0.2
beta_one = 0.9
beta_two = 0.999
adam_eps = 1e-08

bias_one = 1.0 - beta_one**ADAM_STEP
bias_two = 1.0 - beta_two**ADAM_STEP

F32, BF16 = jnp.float32, jnp.bfloat16
CORES = 2
CHUNKS = (3, 4, 5, 2)
MIB = 1 << 20

VMEM = pl.BlockSpec(memory_space=pltpu.VMEM)
SMEM = pl.BlockSpec(memory_space=pltpu.SMEM)
HBM = pl.BlockSpec(memory_space=pltpu.HBM)


def from_root(block, axis, owner):
    block = jnp.where(lax.axis_index(axis) == owner, block, jnp.zeros_like(block))
    return lax.psum(block, axis)


def local_general(activations, out_grads, basis, first_moment, second_moment, reward_codes, token_ids):
    data_count = lax.axis_size("dp")
    tensor_count = lax.axis_size("tensor")
    partial_value = jnp.dot(activations, basis, preferred_element_type=jnp.float32)
    projected = lax.psum(partial_value.astype(jnp.bfloat16), "tensor").astype(jnp.float32)
    unmasked = (token_ids != pad_token).astype(jnp.float32)
    weights = unmasked * jnp.exp(reward_temp * reward_codes.astype(jnp.float32))
    local_total = jnp.sum(weights)
    weighted = (weights[:, None] * projected).astype(jnp.bfloat16)
    raw_grad = lax.dot_general(
        weighted, out_grads, (((0,), (0,)), ((), ())), preferred_element_type=jnp.float32
    )
    normalizer = lax.psum(local_total, "dp")
    grad_rows = lax.psum_scatter(
        raw_grad.astype(jnp.bfloat16), "dp", scatter_dimension=0, tiled=True
    ).astype(jnp.float32)
    token_count = activations.shape[0] * data_count
    gradient = grad_rows * (token_count / normalizer)
    new_first = beta_one * first_moment + (1.0 - beta_one) * gradient
    new_second = beta_two * second_moment + (1.0 - beta_two) * gradient * gradient
    update = (new_first / bias_one / (jnp.sqrt(new_second / bias_two) + adam_eps)).astype(
        jnp.bfloat16
    )
    row_count = basis.shape[0] * tensor_count // data_count
    data_index = lax.axis_index("dp")
    owner_index = data_index * tensor_count // data_count
    owner_rows = from_root(basis, "tensor", owner_index)
    offset = data_index % (data_count // tensor_count) * row_count
    basis_rows = lax.dynamic_slice_in_dim(owner_rows, offset, row_count, 0)
    summed = jnp.dot(
        basis_rows,
        lax.all_gather(update, "dp", axis=0, tiled=True),
        preferred_element_type=jnp.float32,
    )
    return (new_first, new_second, summed.astype(jnp.bfloat16))


def pick(value, width):
    best = 128
    for w in range(128, width + 1, 128):
        if value % w == 0:
            best = w
    return best


def project_kernel(spans, slot_ref, codes_ref, ids_ref, basis_hbm, act_hbm, m_hbm, v_hbm, *refs):
    outs, refs = refs[: len(spans)], refs[len(spans) :]
    weights_ref, sum_ref, mv_ref, turned, basis_buf, basis_sem, act_buf, act_sem = refs[:8]
    m_buf, v_buf, m_sem, v_sem = refs[8:]
    rows = basis_buf.shape[1] // slot_ref.shape[0]
    copy = pltpu.make_async_copy(basis_hbm, basis_buf, basis_sem)
    copy.start()
    copies = []
    for i, (start, count) in enumerate(spans):
        part = pl.ds(start, count)
        copies.append(pltpu.make_async_copy(act_hbm.at[part], act_buf.at[part], act_sem.at[i]))
        copies[-1].start()
    m_copy = pltpu.make_async_copy(m_hbm, m_buf, m_sem)
    v_copy = pltpu.make_async_copy(v_hbm, v_buf, v_sem)
    m_copy.start()
    v_copy.start()
    unmasked = (ids_ref[...] != pad_token).astype(F32)
    weights = unmasked * jnp.exp(reward_temp * codes_ref[...].astype(F32))
    weights_ref[...] = weights
    sum_ref[...] = jnp.broadcast_to(jnp.sum(weights, axis=1, keepdims=True), sum_ref.shape)
    copy.wait()
    flipped = basis_buf[...].T
    for n in range(slot_ref.shape[0]):
        at = pl.multiple_of(slot_ref[n] * rows, rows)
        turned[pl.ds(at, rows), :] = flipped[n * rows : (n + 1) * rows, :]
    largest = max(count for _, count in spans)
    i = 0
    while i < len(spans):
        group = [i]
        while group[-1] + 1 < len(spans) and sum(spans[k][1] for k in group) + spans[group[-1] + 1][1] <= largest:
            group.append(group[-1] + 1)
        for k in group:
            copies[k].wait()
        first, last = spans[group[0]][0], sum(spans[group[-1]])
        product = lax.dot_general(
            turned[...],
            act_buf[first:last, :],
            (((1,), (1,)), ((), ())),
            preferred_element_type=F32,
        ).astype(BF16)
        for k in group:
            start, count = spans[k]
            outs[k][...] = product[:, start - first : start - first + count]
        i = group[-1] + 1
    count = m_buf.shape[0]
    m_copy.wait()
    mv_ref[:count] = m_buf[...].astype(BF16)
    v_copy.wait()
    mv_ref[count:] = v_buf[...].astype(BF16)


def project(slots, codes, ids, basis, activations, first, second, spans):
    tokens, depth = activations.shape
    rank = basis.shape[1]
    rows, full = first.shape
    return pl.pallas_call(
        functools.partial(project_kernel, spans),
        out_shape=[
            *(jax.ShapeDtypeStruct((rank, count), BF16) for _, count in spans),
            jax.ShapeDtypeStruct((1, tokens), F32),
            jax.ShapeDtypeStruct((8, 128), F32),
            jax.ShapeDtypeStruct((2 * rows, full), BF16),
        ],
        in_specs=[SMEM, VMEM, VMEM, HBM, HBM, HBM, HBM],
        out_specs=[VMEM] * (len(spans) + 3),
        scratch_shapes=[
            pltpu.VMEM((rank, depth), BF16),
            pltpu.VMEM((depth, rank), BF16),
            pltpu.SemaphoreType.DMA,
            pltpu.VMEM((tokens, depth), BF16),
            pltpu.SemaphoreType.DMA((len(spans),)),
            pltpu.VMEM((rows, full), F32),
            pltpu.VMEM((rows, full), F32),
            pltpu.SemaphoreType.DMA,
            pltpu.SemaphoreType.DMA,
        ],
        compiler_params=pltpu.CompilerParams(vmem_limit_bytes=52 * MIB),
        cost_estimate=pl.CostEstimate(
            flops=2 * depth * rank * tokens,
            bytes_accessed=2 * (depth * rank + depth * tokens + rank * tokens),
            transcendentals=0,
        ),
        name="project",
    )(slots, codes, ids, basis, activations, first, second)


def small(limit_mib):
    return pltpu.CompilerParams(vmem_limit_bytes=limit_mib * MIB)


def load_kernel(start, source, out_ref, sem):
    parts = sem.shape[0]
    size = out_ref.shape[0] // parts
    copies = [
        pltpu.make_async_copy(
            source.at[pl.ds(start + i * size, size)], out_ref.at[pl.ds(i * size, size)], sem.at[i]
        )
        for i in range(parts)
    ]
    for copy in copies:
        copy.start()
    for copy in copies:
        copy.wait()


def load_rows(source, start, count):
    return pl.pallas_call(
        functools.partial(load_kernel, start),
        out_shape=jax.ShapeDtypeStruct((count, source.shape[1]), source.dtype),
        in_specs=[HBM],
        out_specs=VMEM,
        scratch_shapes=[pltpu.SemaphoreType.DMA((count // 128,))],
        compiler_params=small(16),
        cost_estimate=pl.CostEstimate(
            flops=count * 10**6, bytes_accessed=4 * count * source.shape[1], transcendentals=0
        ),
        name="load",
    )(source)


def gradient_kernel(start, tile, pieces, *refs):
    lefts, grads = refs[:pieces], refs[pieces:-2]
    keep_ref, give_ref = refs[-2:]
    rows, width = keep_ref.shape

    def body(i, _):
        at = pl.multiple_of(i * tile, tile)
        total, piece, row = None, 0, 0
        for left in lefts:
            count = left.shape[1]
            if row == grads[piece].shape[0]:
                piece, row = piece + 1, 0
            term = jnp.dot(
                left[...],
                grads[piece][row : row + count, pl.ds(start + at, tile)],
                preferred_element_type=F32,
            )
            row += count
            total = term if total is None else total + term
        keep_ref[:, pl.ds(at, tile)] = total[:rows].astype(BF16)
        give_ref[:, pl.ds(at, tile)] = total[rows:].astype(BF16)
        return 0

    lax.fori_loop(0, width // tile, body, 0)


def gradient_chunk(lefts, grads, start, width):
    rank = lefts[0].shape[0]
    tokens = sum(piece.shape[0] for piece in grads)
    return pl.pallas_call(
        functools.partial(gradient_kernel, start, pick(width, 512), len(lefts)),
        out_shape=[jax.ShapeDtypeStruct((rank // 2, width), BF16)] * 2,
        in_specs=[VMEM] * (len(lefts) + len(grads)),
        out_specs=[VMEM, VMEM],
        compiler_params=small(4),
        cost_estimate=pl.CostEstimate(
            flops=2 * rank * tokens * width, bytes_accessed=4 * rank * width, transcendentals=0
        ),
        name="gradient",
    )(*lefts, *grads)


def moments(gradient, first, second):
    new_first = beta_one * first + (1.0 - beta_one) * gradient
    new_second = beta_two * second + (1.0 - beta_two) * gradient * gradient
    update = new_first / bias_one / (jnp.sqrt(new_second / bias_two) + adam_eps)
    return new_first, new_second, update


def hub_kernel(
    start, scale_ref, own_ref, came_ref, far_ref, m_ref, v_ref, mv_ref, near_ref, out_ref, mine_ref
):
    rows, width = mine_ref.shape
    total = own_ref[: 2 * rows].astype(F32) + came_ref[: 2 * rows].astype(F32)
    total = total + far_ref[...].astype(F32)
    out_ref[:rows] = total[:rows].astype(BF16)
    mine_ref[...] = total[rows:]
    gradient = total * scale_ref[0, 0]
    cols = slice(start, start + width)
    mv = mv_ref[:, cols].astype(F32)
    near_ref[:rows] = moments(gradient[:rows], mv[:rows], mv[rows:])[2].astype(BF16)
    update = moments(gradient[rows:], m_ref[:, cols], v_ref[:, cols])[2].astype(BF16)
    near_ref[rows:] = update
    out_ref[rows:] = update


def hub_chunk(scale, own, came, far, first, second, moved, start):
    rows, width = first.shape[0], own.shape[1]
    return pl.pallas_call(
        functools.partial(hub_kernel, start),
        out_shape=[
            jax.ShapeDtypeStruct((2 * rows, width), BF16),
            jax.ShapeDtypeStruct((2 * rows, width), BF16),
            jax.ShapeDtypeStruct((rows, width), F32),
        ],
        in_specs=[SMEM] + [VMEM] * 6,
        out_specs=[VMEM] * 3,
        compiler_params=small(4),
        cost_estimate=pl.CostEstimate(
            flops=4000 * rows * width, bytes_accessed=30 * rows * width, transcendentals=0
        ),
        name="hub",
    )(scale, own, came, far, first, second, moved)


def settle_kernel(
    start, scale_ref, hub_ref, mine_ref, m_ref, v_ref, near_ref, across_ref, sent_ref, more_ref, *rest
):
    all_ref, first_out, second_out, first_buf, second_buf, sem = rest[-6:]
    rows, width = mine_ref.shape
    cols = slice(start, start + width)
    hub = hub_ref[0, 0] == 1
    total = jnp.where(hub, mine_ref[...], sent_ref[:rows].astype(F32))
    new_first, new_second, update = moments(
        total * scale_ref[0, 0], m_ref[:, cols], v_ref[:, cols]
    )
    first_buf[...] = new_first
    second_buf[...] = new_second
    copies = [
        pltpu.make_async_copy(first_buf, first_out.at[:, pl.ds(start, width)], sem.at[0]),
        pltpu.make_async_copy(second_buf, second_out.at[:, pl.ds(start, width)], sem.at[1]),
    ]
    for copy in copies:
        copy.start()
    all_ref[:rows] = jnp.where(hub, near_ref[:rows], update.astype(BF16))
    all_ref[rows : 2 * rows] = jnp.where(hub, update.astype(BF16), sent_ref[rows : 2 * rows])
    all_ref[2 * rows :] = jnp.where(hub, across_ref[...], more_ref[...])
    for copy in copies:
        copy.wait()


def settle_chunk(scale, hub, mine, first, second, near, across, sent, more, start, results):
    rows, full = first.shape
    width = mine.shape[1]
    return pl.pallas_call(
        functools.partial(settle_kernel, start),
        out_shape=[
            jax.ShapeDtypeStruct((4 * rows, width), BF16),
            jax.ShapeDtypeStruct((rows, full), F32),
            jax.ShapeDtypeStruct((rows, full), F32),
        ],
        in_specs=[SMEM, SMEM] + [VMEM] * 7 + [HBM] * len(results),
        out_specs=[VMEM, HBM, HBM],
        input_output_aliases={9: 1, 10: 2} if results else {},
        scratch_shapes=[
            pltpu.VMEM((rows, width), F32),
            pltpu.VMEM((rows, width), F32),
            pltpu.SemaphoreType.DMA((2,)),
        ],
        compiler_params=small(4),
        cost_estimate=pl.CostEstimate(
            flops=4000 * rows * width, bytes_accessed=40 * rows * width, transcendentals=0
        ),
        name="settle",
    )(scale, hub, mine, first, second, near, across, sent, more, *results)


def spread_kernel(start, slot_ref, basis_ref, mine_ref, other_ref, *rest):
    out_ref, updates, buf, sem = rest[-4:]
    blocks = slot_ref.shape[0]
    width = mine_ref.shape[1]
    rows = 2 * mine_ref.shape[0] // blocks
    side = blocks // 2
    for n in range(blocks):
        at = slot_ref[n]
        inner = pl.multiple_of((at % side) * rows, rows)
        updates[n * rows : (n + 1) * rows, :] = jnp.where(
            at < side, mine_ref[pl.ds(inner, rows), :], other_ref[pl.ds(inner, rows), :]
        )
    steps = sem.shape[0]
    size = basis_ref.shape[0] // steps
    copies = []
    for i in range(steps):
        part = pl.ds(i * size, size)
        buf[part, :] = jnp.dot(
            basis_ref[part, :], updates[...], preferred_element_type=F32
        ).astype(BF16)
        copies.append(
            pltpu.make_async_copy(
                buf.at[part], out_ref.at[part, pl.ds(start, width)], sem.at[i]
            )
        )
        copies[-1].start()
    for copy in copies:
        copy.wait()


def spread_chunk(slots, basis_rows, mine, other, start, full, results):
    count, rank = basis_rows.shape
    width = mine.shape[1]
    return pl.pallas_call(
        functools.partial(spread_kernel, start),
        out_shape=jax.ShapeDtypeStruct((count, full), BF16),
        in_specs=[SMEM] + [VMEM] * 3 + [HBM] * len(results),
        out_specs=HBM,
        scratch_shapes=[
            pltpu.VMEM((rank, width), BF16),
            pltpu.VMEM((count, width), BF16),
            pltpu.SemaphoreType.DMA((4 if count % 64 == 0 else 1,)),
        ],
        input_output_aliases={4: 0} if results else {},
        compiler_params=small(9),
        cost_estimate=pl.CostEstimate(
            flops=2 * count * rank * width,
            bytes_accessed=2 * (count * rank + rank * width + count * width),
            transcendentals=0,
        ),
        name="spread",
    )(slots, basis_rows, mine, other, *results)


def token_pieces(tokens):
    if tokens % (6 * 128) == 0:
        sizes = [tokens // 3, tokens // 3, tokens // 6, tokens // 6]
    else:
        count = tokens // 128
        sizes = [(count // 4 + (i < count % 4)) * 128 for i in range(4)]
    return [(sum(sizes[:i]), size) for i, size in enumerate(sizes)]


def local_line(activations, out_grads, basis, first_moment, second_moment, reward_codes, token_ids):
    data_count = lax.axis_size("dp")
    tensor_count = lax.axis_size("tensor")
    data_index = lax.axis_index("dp")
    tensor_index = lax.axis_index("tensor")
    chips = data_count // CORES
    chip, core = data_index // CORES, data_index % CORES
    tokens = activations.shape[0]
    full = out_grads.shape[1]
    rows = first_moment.shape[0]

    def on_chips(pairs):
        return [(a * CORES + c, b * CORES + c) for a, b in pairs for c in range(CORES)]

    inward = on_chips([(0, 1), (3, 2)])
    outward = on_chips([(1, 0), (2, 3)])
    middle = on_chips([(1, 2), (2, 1)])
    sibling = [(i, i ^ 1) for i in range(data_count)]
    hub = ((chip == 1) | (chip == 2)).astype(jnp.int32).reshape(1, 1)

    block = jnp.arange(data_count, dtype=jnp.int32)
    block_chip = block // CORES
    far = (block_chip // 2 != chip // 2).astype(jnp.int32)
    is_hub = ((block_chip == 1) | (block_chip == 2)).astype(jnp.int32)
    slots = ((block % CORES) ^ core).astype(jnp.int32) * chips + 2 * far + is_hub

    row_count = basis.shape[0] * tensor_count // data_count
    per_owner = data_count // tensor_count
    owner = data_index // per_owner
    basis_rows = lax.dynamic_slice_in_dim(basis, data_index % per_owner * row_count, row_count, 0)
    basis_rows = jnp.where(tensor_index == owner, basis_rows, jnp.zeros_like(basis_rows))
    bits = [1 << b for b in range(tensor_count.bit_length() - 1)]
    *parts, weights, normalizer, packed = project(
        slots,
        reward_codes.reshape(1, tokens),
        token_ids.reshape(1, tokens),
        basis,
        activations,
        first_moment,
        second_moment,
        token_pieces(tokens),
    )
    got = [None] * len(parts)
    for step in range(len(bits)):
        for i, part in enumerate(parts):
            bit = bits[step] if i % 2 == 0 else bits[-1 - step]
            if step:
                part = parts[i] = (part.astype(F32) + got[i].astype(F32)).astype(BF16)
            pairs = [(t, t ^ bit) for t in range(tensor_count)]
            got[i] = lax.ppermute(part, "tensor", pairs)

    for b in range(data_count.bit_length() - 1):
        pairs = [(i, i ^ (1 << b)) for i in range(data_count)]
        normalizer = normalizer + lax.ppermute(normalizer, "dp", pairs)
    scale = (tokens * data_count) / normalizer[:1, :1]

    lefts = []
    for (start, count), part, other in zip(token_pieces(tokens), parts, got):
        total = part.astype(F32) + other.astype(F32)
        lefts.append((weights[:, start : start + count] * total).astype(BF16))

    moved = lax.ppermute(packed, "dp", inward)
    out_grads, basis_rows, hub, slots = lax.optimization_barrier(
        (out_grads, basis_rows, hub, slots)
    )
    grads = []
    spans = token_pieces(tokens)
    cut = spans[2][0]
    for start, count in ((0, cut), (cut, tokens - cut)):
        grads.append(load_rows(out_grads, start, count))

    for bit in bits:
        pairs = [
            (d * tensor_count + (d // per_owner ^ s), d * tensor_count + (d // per_owner ^ s ^ bit))
            for d in range(data_count)
            for s in range(bit)
        ]
        basis_rows = basis_rows + lax.ppermute(basis_rows, ("dp", "tensor"), pairs)

    unit = full // sum(CHUNKS)
    starts = [unit * sum(CHUNKS[:i]) for i in range(len(CHUNKS))]
    settled, spread = (), ()
    for start, size in zip(starts, CHUNKS):
        keep, give = gradient_chunk(lefts, grads, start, unit * size)
        mine = keep + lax.ppermute(give, "dp", sibling)
        came = lax.ppermute(mine, "dp", inward)
        across = lax.ppermute(mine[2 * rows :] + came[2 * rows :], "dp", middle)
        near, ready, held = hub_chunk(
            scale, mine, came, across, first_moment, second_moment, moved, start
        )
        beyond = lax.ppermute(near, "dp", middle)
        sent = lax.ppermute(ready, "dp", outward)
        more = lax.ppermute(beyond, "dp", outward)
        updates, *settled = settle_chunk(
            scale, hub, held, first_moment, second_moment, near, beyond, sent, more, start, settled
        )
        other = lax.ppermute(updates, "dp", sibling)
        spread = (spread_chunk(slots, basis_rows, updates, other, start, full, spread),)
    return (*settled, *spread)


def staged(*args):
    return local_line(*args)


def solution(mesh):
    data_count, tensor_count = mesh.shape["dp"], mesh.shape["tensor"]
    line = data_count == 4 * CORES and tensor_count > 1 and tensor_count & (tensor_count - 1) == 0
    line = line and data_count % tensor_count == 0
    return jax.shard_map(
        staged if line else local_general,
        mesh=mesh,
        in_specs=(
            P("dp", "tensor"),
            P("dp", "tensor"),
            P("tensor", None),
            P("dp", "tensor"),
            P("dp", "tensor"),
            P("dp"),
            P("dp"),
        ),
        out_specs=(P("dp", "tensor"), P("dp", "tensor"), P("dp", "tensor")),
        check_vma=False,
    )
```
